32 devices in a mesh: band: 8 (over z, x), lev: 4 (over y, core).
Axes of the slice: x: 2, y: 2, z: 4, core: 2. Of those that a mesh axis runs over, the one named last changes fastest.
Arguments:
- checkpoints: float32 [4, 4, 32, 2, 256, 256], P(None, None, 'lev', None, 'band'), may hold values from -0.4 to 0.4
- final_cot: float32 [4, 32, 2, 256, 256], P(None, 'lev', None, 'band'), may hold values from -6 to 6
- obs_cot: float32 [4, 4, 32, 256, 512], P(None, None, None, 'band', 'lev'), may hold values from -0.2 to 0.2
- obs_time: int32 [4], replicated, may hold values from 0 to 3
- wave_order: int32 [256], replicated, may hold values from 0 to 255, each once
- legendre: bfloat16 [256, 256, 256], P('band'), may hold values from -0.375 to 0.375
- w_in: bfloat16 [128, 512], replicated, may hold values from -0.5 to 0.5
- w_out: bfloat16 [512, 128], replicated, may hold values from -0.25 to 0.25
- bias: float32 [512], replicated, may hold values from -3 to 3
Outputs:
- grad_state: float32 [4, 32, 2, 256, 256], P(None, 'lev', None, 'band')
- grad_w_in: float32 [128, 512], replicated
- grad_w_out: float32 [512, 128], replicated
- grad_bias: float32 [512], replicated
The draws below stay inside these ranges and needn't reach their ends.
Inputs may be any that keep to these rules, and one draw needn't show every extreme that they name: `obs_time`: each number names a step of the rollout. `wave_order`: each of the 256 zonal wavenumbers once.
All inputs are finite; a program needn't handle non-finite values.
Results may differ from the reference program's by a relative error of at most 0.014.
Values may be sent and summed in bfloat16 or wider, within the bound.
A program may use at most 192 MiB of HBM per device.

```python
import jax
import jax.numpy as jnp
from jax import lax

M = 256
LAT = 256
LON = 512
LEV = 32
VARS = 4
HID = 512
STEPS = 4
NOBS = 4


def plant(result, stream_key, least, largest):
    longest = result.shape.index(max(result.shape))
    spots = []
    for shift in (0, 1):
        where = [jax.random.randint(jax.random.fold_in(stream_key, axis), (), 0, length) for axis, length in enumerate(result.shape)]
        where[longest] = (where[longest] + shift) % result.shape[longest]
        spots.append(tuple(where))
    return result.at[spots[0]].set(least).at[spots[1]].set(largest)


def steps_of(rng, shape, shards, smallest, top_value):
    level = 1.0
    for position, parts in shards:
        steps = jax.random.uniform(jax.random.fold_in(jax.random.fold_in(rng, 6), position), (parts,), jnp.float32, smallest / len(shards), top_value / len(shards))
        level = level * jnp.repeat(jnp.exp(steps), shape[position] // parts).reshape((-1,) + (1,) * (len(shape) - 1 - position))
    return level


def bell_draw(stream_key, shape, width, limit, shards=(), kind=jnp.bfloat16):
    array = width * jax.random.normal(stream_key, shape, jnp.float32)
    if shards:
        array = array * steps_of(stream_key, shape, shards, -0.22, 0.18)
    return jnp.clip(array, -limit, limit).astype(kind)


def setup_inputs(seed: int = 0) -> dict:
    arg_keys = jax.random.split(jax.random.key(seed), 10)
    checkpoints = bell_draw(arg_keys[0], (STEPS, VARS, LEV, 2, M, M), 0.05, 0.4, ((2, 4), (4, 8)), jnp.float32)
    final_cot = bell_draw(arg_keys[1], (VARS, LEV, 2, M, M), 1.0, 6.0, ((1, 4), (3, 8)), jnp.float32)
    obs_cot = bell_draw(arg_keys[2], (NOBS, VARS, LEV, LAT, LON), 0.03, 0.2, ((3, 8), (4, 4)), jnp.float32)
    obs_time = plant(jax.random.randint(arg_keys[3], (NOBS,), 0, STEPS), jax.random.fold_in(arg_keys[3], 1), 0, STEPS - 1).astype(jnp.int32)
    wave_order = jax.random.permutation(arg_keys[4], M).astype(jnp.int32)
    legendre = bell_draw(arg_keys[5], (M, LAT, M), M ** -0.5, 0.375, ((0, 8),))
    w_in = bell_draw(arg_keys[6], (VARS * LEV, HID), (VARS * LEV) ** -0.5, 0.5)
    w_out = bell_draw(arg_keys[7], (HID, VARS * LEV), HID ** -0.5, 0.25)
    bias = bell_draw(arg_keys[8], (HID,), 0.5, 3.0, (), jnp.float32)
    return dict(checkpoints=checkpoints, final_cot=final_cot, obs_cot=obs_cot, obs_time=obs_time, wave_order=wave_order, legendre=legendre, w_in=w_in, w_out=w_out, bias=bias)


highest = lax.Precision.HIGHEST
dt_scale = 1.0


def lowered(values):
    return lax.optimization_barrier(values.astype(jnp.bfloat16)).astype(jnp.float32)


def tables(wave_order, lon_count):
    longitude = jnp.arange(lon_count, dtype=jnp.int32)
    phase_index = (wave_order[:, None] * longitude[None, :]) % lon_count
    angles = (2.0 * jnp.pi / lon_count) * phase_index.astype(jnp.float32)
    return lowered(jnp.cos(angles)), lowered(jnp.sin(angles))


def synth_legendre(masked, spectral):
    return lowered(jnp.einsum('rjn,vlcrn->vlcrj', masked, lowered(spectral), precision=highest))


def synth_fourier(coefficients, factor, cosine_table, sine_table):
    real_part = coefficients[:, :, 0] * factor[None, None, :, None]
    imag_part = coefficients[:, :, 1] * factor[None, None, :, None]
    return (jnp.einsum('vlrj,ro->vljo', real_part, cosine_table, precision=highest)
            - jnp.einsum('vlrj,ro->vljo', imag_part, sine_table, precision=highest))


def adjoint_fourier(grid_field, factor, cosine_table, sine_table):
    real_part = jnp.einsum('vljo,ro->vlrj', grid_field, cosine_table, precision=highest) * factor[:, None]
    imag_part = -jnp.einsum('vljo,ro->vlrj', grid_field, sine_table, precision=highest) * factor[:, None]
    return lowered(jnp.stack([real_part, imag_part], axis=2))


def adjoint_legendre(masked, coefficients):
    return jnp.einsum('rjn,vlcrj->vlcrn', masked, coefficients, precision=highest)


def reference(checkpoints, final_cot, obs_cot, obs_time, wave_order, legendre, w_in, w_out, bias):
    degrees = jnp.arange(M, dtype=jnp.int32)
    upper_mask = (degrees[None, None, :] >= wave_order[:, None, None]).astype(jnp.float32)
    masked = legendre.astype(jnp.float32) * upper_mask
    cosine_table, sine_table = tables(wave_order, LON)
    weight_m = jnp.where(wave_order == 0, 1.0, 2.0).astype(jnp.float32)
    inverse_lon = jnp.full((M,), 1.0 / LON, jnp.float32)
    degree_float = degrees.astype(jnp.float32)
    damping = 1.0 / (1.0 + 2.0 * degree_float * (degree_float + 1.0) / (M * M))
    feature_count = VARS * LEV
    column_count = LAT * LON
    adjoint = final_cot
    grad_w_in = jnp.zeros((feature_count, HID), jnp.float32)
    grad_w_out = jnp.zeros((HID, feature_count), jnp.float32)
    grad_bias = jnp.zeros((HID,), jnp.float32)
    for step in reversed(range(STEPS)):
        damped = damping * adjoint
        state_grid = synth_fourier(synth_legendre(masked, checkpoints[step]), weight_m, cosine_table, sine_table)
        features = state_grid.astype(jnp.bfloat16).reshape(feature_count, column_count)
        tangent_grid = synth_fourier(synth_legendre(masked, dt_scale * damped), inverse_lon, cosine_table, sine_table)
        tangent = tangent_grid.astype(jnp.bfloat16).reshape(feature_count, column_count)
        preact = jnp.dot(w_in.T, features, preferred_element_type=jnp.float32) + bias[:, None]
        logistic = jax.nn.sigmoid(preact)
        hidden = (preact * logistic).astype(jnp.bfloat16)
        hidden_grad = jnp.dot(w_out, tangent, preferred_element_type=jnp.float32)
        preact_grad = hidden_grad * (logistic * (1.0 + preact * (1.0 - logistic)))
        preact_low = preact_grad.astype(jnp.bfloat16)
        grad_w_out = grad_w_out + jnp.dot(hidden, tangent.T, preferred_element_type=jnp.float32)
        grad_w_in = grad_w_in + jnp.dot(features, preact_low.T, preferred_element_type=jnp.float32)
        grad_bias = grad_bias + jnp.sum(preact_grad, axis=1)
        column_grad = jnp.dot(w_in, preact_low, preferred_element_type=jnp.float32).reshape(VARS, LEV, LAT, LON)
        obs_weight = (obs_time == step).astype(jnp.float32)
        column_grad = column_grad + jnp.einsum('i,ivljo->vljo', obs_weight, obs_cot, precision=highest)
        back = adjoint_fourier(lowered(column_grad), weight_m, cosine_table, sine_table)
        adjoint = damped + adjoint_legendre(masked, back)
    return adjoint, grad_w_in, grad_w_out, grad_bias
```

```python
import functools

import jax
import jax.numpy as jnp
from jax import lax
from jax.experimental import pallas as pl
from jax.experimental.pallas import tpu as pltpu
from jax.sharding import PartitionSpec as P

dt_scale = 1.0
F32 = jnp.float32
BF16 = jnp.bfloat16
MESH = pl.DeviceIdType.MESH
LANES = 128


def dot(a, b):
    return jnp.dot(a, b, preferred_element_type=F32)


def dot_nt(a, b):
    return lax.dot_general(a, b, (((1,), (1,)), ((), ())), preferred_element_type=F32)


class Sizes:
    def __init__(self, bands, levs, steps, fields, levels, waves, wave_count, lat, lon, nobs, hidden):
        self.B, self.LV, self.S, self.NO = bands, levs, steps, nobs
        self.V, self.L, self.R, self.N = fields, levels, waves, wave_count
        self.J, self.O, self.H = lat, lon, hidden
        self.RP = waves // 2
        self.RT = self.RP * bands
        self.JJ = min(16, lat)
        self.Q = lat // self.JJ
        self.VL = fields * levels
        self.C = 4 * self.VL
        self.F = self.VL * levs
        self.ND = bands * levs
        self.HD = hidden // self.ND
        self.PITCH = self.JJ + 8
        self.OPITCH = self.F + 8
        self.ROWS = self.VL * 2 * waves
        self.G = min(8, self.JJ)
        self.HC = min(256, hidden)


def kernel(
    z, ck, fc, obs, leg, obs_time, wave, damp, tab_t, tab_w, w_in_t, w_in, w_out, bias,
    out, gout,
    tab, adj, tsend, trecv, fsend, frecv, bsend, brecv,
    lf_send, lf_recv, lt_send, lt_recv, lg_send, lg_recv,
    fs, fs2, cstage, ostage, obs_all, obs_s, acc_in, acc_out, acc_b,
    rs_send, rs_recv, ag_send, ag_recv,
    t_s, t_r, f_s, f_r, b_s, b_r, lf_s, lf_r, lt_s, lt_r, lg_s, lg_r, rs_s, rs_r, ag_s, ag_r,
    ck_sem, fc_sem, obs_sem, leg_sem, out_sem, g_sem,
):
    me_b = lax.axis_index("band")
    me_l = lax.axis_index("lev")
    me = me_b * z.LV + me_l

    def to_band(src, dst, ssem, rsem, b):
        return pltpu.make_async_remote_copy(
            src_ref=src, dst_ref=dst, send_sem=ssem, recv_sem=rsem,
            device_id=(b, me_l), device_id_type=MESH,
        )

    def to_lev(src, dst, ssem, rsem, v):
        return pltpu.make_async_remote_copy(
            src_ref=src, dst_ref=dst, send_sem=ssem, recv_sem=rsem,
            device_id=(me_b, v), device_id_type=MESH,
        )

    def others(count, own, body):
        def step(d, _):
            body(lax.rem(own + d, count))
            return 0

        lax.fori_loop(1, count, step, 0)

    def band_send(send, recv, ssem, rsem, q):
        others(z.B, me_b, lambda b: to_band(
            send.at[b, q], recv.at[me_b, q], ssem.at[q, b], rsem.at[q, me_b], b).start())
        recv[me_b, q] = send[me_b, q]

    def band_wait_recv(send, recv, ssem, rsem, q):
        others(z.B, me_b, lambda b: to_band(
            send.at[b, q], recv.at[b, q], ssem.at[q, b], rsem.at[q, b], b).wait_recv())

    def band_wait_send(send, recv, ssem, rsem, q):
        others(z.B, me_b, lambda b: to_band(
            send.at[b, q], recv.at[b, q], ssem.at[q, b], rsem.at[q, b], b).wait_send())

    def feat_send(par):
        others(z.B, me_b, lambda b: to_band(
            fsend.at[b], frecv.at[par, me_b], f_s.at[b], f_r.at[par, me_b], b).start())
        frecv[par, me_b] = fsend[me_b]

    def feat_wait_recv(par):
        others(z.B, me_b, lambda b: to_band(
            fsend.at[b], frecv.at[par, b], f_s.at[b], f_r.at[par, b], b).wait_recv())

    def feat_wait_send():
        others(z.B, me_b, lambda b: to_band(
            fsend.at[b], frecv.at[0, b], f_s.at[b], f_r.at[0, b], b).wait_send())

    def lev_send(send, recv, ssem, rsem, q):
        others(z.LV, me_l, lambda v: to_lev(
            send.at[v, q], recv.at[me_l, q], ssem.at[q, v], rsem.at[q, me_l], v).start())
        recv[me_l, q] = send[me_l, q]

    def lev_wait_recv(send, recv, ssem, rsem, q):
        others(z.LV, me_l, lambda v: to_lev(
            send.at[v, q], recv.at[v, q], ssem.at[q, v], rsem.at[q, v], v).wait_recv())

    def lev_wait_send(send, recv, ssem, rsem, q):
        others(z.LV, me_l, lambda v: to_lev(
            send.at[v, q], recv.at[v, q], ssem.at[q, v], rsem.at[q, v], v).wait_send())

    def ck_copy(k, h):
        return pltpu.make_async_copy(
            ck.at[k, :, pl.ds(h * LANES, LANES)], cstage.at[h], ck_sem.at[h])

    def fc_copy(h):
        return pltpu.make_async_copy(
            fc.at[:, pl.ds(h * LANES, LANES)], ostage.at[h], fc_sem.at[h])

    def out_copy(h):
        return pltpu.make_async_copy(
            ostage.at[h], out.at[:, pl.ds(h * LANES, LANES)], out_sem.at[h])

    halves = z.N // LANES
    bj = z.B * z.JJ
    if z.Q == 1:
        leg_copies = [pltpu.make_async_copy(leg, tab.at[:, 0], leg_sem.at[0])]
    else:
        leg_copies = [
            pltpu.make_async_copy(
                leg.at[:, pl.ds(b * z.J + q * z.JJ, z.JJ), :],
                tab.at[:, q, pl.ds(b * z.JJ, z.JJ), :],
                leg_sem.at[b * z.Q + q],
            )
            for b in range(z.B)
            for q in range(z.Q)
        ]
    obs_copy = pltpu.make_async_copy(obs, obs_all, obs_sem.at[0])
    for h in range(halves):
        ck_copy(z.S - 1, h).start()
    for c in leg_copies:
        c.start()
    for h in range(halves):
        fc_copy(h).start()
    obs_copy.start()

    half_c = 2 * z.VL
    degree = lax.broadcasted_iota(jnp.int32, (half_c, z.N), 1)

    def upper(rp, r2):
        return degree >= wave[me_b * z.R + 2 * rp + r2]

    def rows_of(stage, rp):
        parts = []
        for r2 in range(2):
            for p in range(2):
                start = p * z.R + 2 * rp + r2
                parts.append(jnp.concatenate(
                    [stage[h, pl.ds(start, z.VL, stride=2 * z.R), :] for h in range(halves)], axis=1))
        return jnp.concatenate(parts, axis=0)

    lane = lax.broadcasted_iota(jnp.int32, (z.Q * bj, z.C), 1)

    def legendre(s, rp, send):
        masked = jnp.concatenate(
            [jnp.where(upper(rp, r2), s[r2 * half_c:(r2 + 1) * half_c], 0.0) for r2 in range(2)],
            axis=0).astype(BF16)
        sums = [dot_nt(tab[2 * rp + r2].reshape(z.Q * bj, z.N), masked) for r2 in range(2)]
        sums = jnp.where(lane < half_c, sums[0], sums[1])
        for q in range(z.Q):
            for b in range(z.B):
                row = q * bj + b * z.JJ
                send[b, q, rp] = sums[row:row + z.JJ].astype(BF16)

    def features_legendre():
        def body(rp, _):
            legendre(rows_of(cstage, rp), rp, fsend)
            return 0

        lax.fori_loop(0, z.RP, body, 0, unroll=2)

    def tangent_legendre():
        def body(rp, _):
            damped = damp[...] * adj[rp]
            adj[rp] = damped
            legendre(dt_scale * damped, rp, tsend)
            return 0

        lax.fori_loop(0, z.RP, body, 0, unroll=2)

    def fourier(recv, q, table, scale, send):
        def convert(b, _):
            block = recv[b, q].astype(F32)
            for rp in range(z.RP):
                row = pl.multiple_of((b * z.RP + rp) * z.PITCH, 8)
                fs[pl.ds(row, z.JJ), :] = block[rp]
            return 0

        lax.fori_loop(0, z.B, convert, 0)

        def group(g, _):
            parts = []
            for i in range(z.G):
                at = fs[pl.ds(g * z.G + i, z.RT, stride=z.PITCH), :].T.astype(BF16)
                parts.append(jnp.concatenate(
                    [at[c * z.VL:(c + 1) * z.VL] for c in range(4)], axis=1))
            y = dot(jnp.concatenate(parts, axis=0), table[...])
            if scale is not None:
                y = y * scale
            y = y.astype(BF16)
            for v in range(z.LV):
                for i in range(z.G):
                    send[v, q, g * z.G + i] = y[i * z.VL:(i + 1) * z.VL, v * z.O:(v + 1) * z.O]
            return 0

        lax.fori_loop(0, z.JJ // z.G, group, 0)

    def adjoint_fourier(q):
        def group(g, _):
            x = jnp.concatenate([
                jnp.concatenate([lg_recv[v, q, g * z.G + i] for v in range(z.LV)], axis=1)
                for i in range(z.G)], axis=0)
            y = dot_nt(x, tab_w[...])
            for i in range(z.G):
                yi = y[i * z.VL:(i + 1) * z.VL]
                st = jnp.concatenate([yi[:, c * z.RT:(c + 1) * z.RT] for c in range(4)], axis=0)
                fs2[pl.ds(g * z.G + i, z.RT, stride=z.PITCH), :] = st.T
            return 0

        lax.fori_loop(0, z.JJ // z.G, group, 0)

        def convert(b, _):
            for rp in range(z.RP):
                row = pl.multiple_of((b * z.RP + rp) * z.PITCH, 8)
                bsend[b, q, rp] = fs2[pl.ds(row, z.JJ), :].astype(BF16)
            return 0

        lax.fori_loop(0, z.B, convert, 0)

    def adjoint_legendre(q):
        def body(rp, _):
            b_t = jnp.concatenate(
                [brecv[b, q, rp].astype(F32) for b in range(z.B)], axis=0).T.astype(BF16)
            for r2 in range(2):
                rows = slice(r2 * half_c, (r2 + 1) * half_c)
                grad = dot(b_t[rows], tab[2 * rp + r2, q])
                adj[rp, rows] = adj[rp, rows] + jnp.where(upper(rp, r2), grad, 0.0)
            return 0

        lax.fori_loop(0, z.RP, body, 0, unroll=2)

    def observations(k):
        weights = [jnp.where(obs_time[i] == k, 1.0, 0.0).astype(F32) for i in range(z.NO)]

        def body(f, _):
            v, rest = f // z.LV // z.L, lax.rem(f, z.LV * z.L)
            row = (rest // z.L) * z.VL + v * z.L + lax.rem(rest, z.L)
            total = weights[0] * obs_all[0, f]
            for i in range(1, z.NO):
                total = total + weights[i] * obs_all[i, f]
            obs_s[pl.ds(row, z.J, stride=z.OPITCH), :] = total
            return 0

        lax.fori_loop(0, z.F, body, 0, unroll=4)

    ng = min(4, z.JJ)

    def network(q):
        def group(g, _):
            def columns(ref):
                return jnp.concatenate([
                    jnp.concatenate([ref[v, q, g * ng + i] for v in range(z.LV)], axis=0)
                    for i in range(ng)], axis=1)

            x = columns(lf_recv)
            t = columns(lt_recv)
            grad = None
            for h in range(0, z.H, z.HC):
                rows = slice(h, h + z.HC)
                b = bias[rows]
                pre = dot(w_in_t[rows], x) + jnp.concatenate([b] * ng, axis=1)
                logistic = 0.5 * jnp.tanh(0.5 * pre) + 0.5
                hid = pre * logistic
                pg = dot(w_out[rows], t) * (logistic + hid * (1.0 - logistic))
                low = pg.astype(BF16)
                acc_out[rows] += dot_nt(hid.astype(BF16), t)
                acc_in[rows] += dot_nt(low, x)
                total = pg[:, :z.O]
                for i in range(1, ng):
                    total = total + pg[:, i * z.O:(i + 1) * z.O]
                acc_b[rows] += total
                part = dot(w_in[:, rows], low)
                grad = part if grad is None else grad + part
            for i in range(ng):
                j = q * z.JJ + g * ng + i
                row = pl.multiple_of(j * z.OPITCH, 8)
                col = grad[:, i * z.O:(i + 1) * z.O] + obs_s[pl.ds(row, z.F), :]
                col = col.astype(BF16)
                for v in range(z.LV):
                    lg_send[v, q, g * ng + i] = col[v * z.VL:(v + 1) * z.VL]
            return 0

        lax.fori_loop(0, z.JJ // ng, group, 0)

    def to_device(src, dst, ssem, rsem, d):
        return pltpu.make_async_remote_copy(
            src_ref=src, dst_ref=dst, send_sem=ssem, recv_sem=rsem,
            device_id=(d // z.LV, lax.rem(d, z.LV)), device_id_type=MESH,
        )

    def reduce_send():
        for i, acc in enumerate((acc_in, acc_out, acc_b)):
            for d in range(z.ND):
                rs_send[d, i] = acc[d * z.HD:(d + 1) * z.HD].astype(BF16)
        rs_recv[me] = rs_send[me]
        others(z.ND, me, lambda d: to_device(
            rs_send.at[d], rs_recv.at[me], rs_s.at[d], rs_r.at[me], d).start())

    def gather_send():
        others(z.ND, me, lambda d: to_device(
            rs_send.at[d], rs_recv.at[d], rs_s.at[d], rs_r.at[d], d).wait())
        total = rs_recv[0].astype(F32)
        for d in range(1, z.ND):
            total = total + rs_recv[d].astype(F32)
        total = total.astype(BF16)
        ag_send[...] = total
        ag_recv[me] = total
        others(z.ND, me, lambda d: to_device(
            ag_send, ag_recv.at[me], ag_s.at[d], ag_r.at[me], d).start())

    def gather_wait():
        others(z.ND, me, lambda d: to_device(
            ag_send, ag_recv.at[d], ag_s.at[d], ag_r.at[d], d).wait())

    acc_in[...] = jnp.zeros_like(acc_in)
    acc_out[...] = jnp.zeros_like(acc_out)
    acc_b[...] = jnp.zeros_like(acc_b)

    for h in range(halves):
        ck_copy(z.S - 1, h).wait()
    for c in leg_copies:
        c.wait()
    features_legendre()
    feat_send((z.S - 1) % 2)
    if z.S > 1:
        for h in range(halves):
            ck_copy(z.S - 2, h).start()
    for h in range(halves):
        fc_copy(h).wait()

    def initial(rp, _):
        adj[rp] = rows_of(ostage, rp)
        return 0

    lax.fori_loop(0, z.RP, initial, 0)

    tang = (tsend, trecv, t_s, t_r)
    back = (bsend, brecv, b_s, b_r)
    lt = (lt_send, lt_recv, lt_s, lt_r)
    lf = (lf_send, lf_recv, lf_s, lf_r)
    lg = (lg_send, lg_recv, lg_s, lg_r)

    def step(i, _):
        k = z.S - 1 - i
        par = lax.rem(k, 2)
        tangent_legendre()
        for q in range(z.Q):
            band_send(*tang, q)
        feat_wait_recv(par)
        for q in range(z.Q):
            fourier(frecv.at[par], q, tab_w, None, lf_send)
            lev_send(*lf, q)

        @pl.when(k > 0)
        def _():
            for h in range(halves):
                ck_copy(k - 1, h).wait()
            feat_wait_send()
            features_legendre()
            feat_send(1 - par)

        @pl.when(k > 1)
        def _():
            for h in range(halves):
                ck_copy(k - 2, h).start()

        @pl.when(i == 0)
        def _():
            obs_copy.wait()

        observations(k)

        def do_t(q):
            band_wait_recv(*tang, q)
            fourier(trecv, q, tab_t, 1.0 / (z.O * z.LV), lt_send)
            lev_send(*lt, q)

        def do_n(q):
            lev_wait_recv(*lf, q)
            lev_wait_recv(*lt, q)
            network(q)
            lev_send(*lg, q)

        def do_b(q):
            lev_wait_recv(*lg, q)

            @pl.when(i > 0)
            def _():
                band_wait_send(*back, q)

            adjoint_fourier(q)
            band_send(*back, q)

        do_t(0)
        do_n(0)
        for q in range(1, z.Q):
            do_t(q)
            do_b(q - 1)
            do_n(q)

        @pl.when(k == 0)
        def _():
            reduce_send()

        do_b(z.Q - 1)

        @pl.when(k == 0)
        def _():
            gather_send()

        for q in range(z.Q):
            band_wait_recv(*back, q)
            adjoint_legendre(q)
        for q in range(z.Q):
            band_wait_send(*tang, q)
            lev_wait_send(*lf, q)
            lev_wait_send(*lt, q)
            lev_wait_send(*lg, q)
        return 0

    lax.fori_loop(0, z.S, step, 0)

    def final(rp, _):
        for r2 in range(2):
            for p in range(2):
                start = p * z.R + 2 * rp + r2
                c = r2 * half_c + p * z.VL
                for h in range(halves):
                    ostage[h, pl.ds(start, z.VL, stride=2 * z.R), :] = (
                        adj[rp, c:c + z.VL, h * LANES:(h + 1) * LANES])
        return 0

    lax.fori_loop(0, z.RP, final, 0)
    for h in range(halves):
        out_copy(h).start()
    gather_wait()
    gather_copy = pltpu.make_async_copy(ag_recv, gout, g_sem.at[0])
    gather_copy.start()
    feat_wait_send()
    for q in range(z.Q):
        band_wait_send(*back, q)
    for h in range(halves):
        out_copy(h).wait()
    gather_copy.wait()


def shards(checkpoints, final_cot, obs_cot, obs_time, wave_order, legendre, w_in, w_out, bias):
    local_waves, lat_count, wave_count = legendre.shape
    fields, levels = final_cot.shape[:2]
    z = Sizes(
        lax.axis_size("band"), lax.axis_size("lev"), checkpoints.shape[0], fields, levels,
        local_waves, wave_count, obs_cot.shape[3], obs_cot.shape[4], obs_cot.shape[0],
        w_in.shape[1])
    lon_count = z.O * z.LV
    order = wave_order.reshape(z.RT, 2).T[:, None, :, None]
    longitude = jnp.arange(lon_count, dtype=jnp.int32)
    phase = (order * longitude) % lon_count
    angles = 2.0 * jnp.pi / lon_count * phase.astype(F32)
    table = jnp.concatenate(
        [jnp.cos(angles).astype(BF16), -jnp.sin(angles).astype(BF16)], axis=1)
    weight = jnp.where(order == 0, 1.0, 2.0).astype(BF16)
    tab_w = (table * weight).reshape(4 * z.RT, lon_count)
    tab_t = table.reshape(4 * z.RT, lon_count)
    degree = jnp.arange(wave_count, dtype=jnp.int32).astype(F32)
    damp = (1.0 / (1.0 + 2.0 * degree * (degree + 1.0) / (wave_count * wave_count)))[None]

    def to_wire(w, axis):
        shape = w.shape[:axis] + (fields, z.LV, levels) + w.shape[axis + 1:]
        return jnp.swapaxes(w.reshape(shape), axis, axis + 1).reshape(w.shape)

    def from_wire(w, axis):
        shape = w.shape[:axis] + (z.LV, fields, levels) + w.shape[axis + 1:]
        return jnp.swapaxes(w.reshape(shape), axis, axis + 1).reshape(w.shape)

    w_in_p = to_wire(w_in, 0)
    w_out_p = to_wire(w_out, 1)
    any_space = pl.BlockSpec(memory_space=pl.ANY)
    smem = pl.BlockSpec(memory_space=pltpu.SMEM)
    vmem = pl.BlockSpec(memory_space=pltpu.VMEM)
    dma = pltpu.SemaphoreType.DMA
    band_buf = pltpu.VMEM((z.B, z.Q, z.RP, z.JJ, z.C), BF16)
    lev_buf = pltpu.VMEM((z.LV, z.Q, z.JJ, z.VL, z.O), BF16)
    halves = z.N // LANES
    reduce_buf = pltpu.VMEM((z.ND, 3, z.HD, z.F), BF16)
    scratch = [
        pltpu.VMEM((z.R, z.Q, z.B * z.JJ, z.N), BF16),
        pltpu.VMEM((z.RP, z.C, z.N), F32),
        band_buf, band_buf, band_buf,
        pltpu.VMEM((2, z.B, z.Q, z.RP, z.JJ, z.C), BF16),
        band_buf, band_buf,
        lev_buf, lev_buf, lev_buf, lev_buf, lev_buf, lev_buf,
        pltpu.VMEM((z.RT * z.PITCH, z.C), F32),
        pltpu.VMEM((z.RT * z.PITCH, z.C), F32),
        pltpu.VMEM((halves, z.ROWS, LANES), F32),
        pltpu.VMEM((halves, z.ROWS, LANES), F32),
        pltpu.VMEM((z.NO, z.F, z.J, z.O), F32),
        pltpu.VMEM((z.J * z.OPITCH, z.O), F32),
        pltpu.VMEM((z.H, z.F), F32), pltpu.VMEM((z.H, z.F), F32), pltpu.VMEM((z.H, z.O), F32),
        reduce_buf, reduce_buf,
        pltpu.VMEM((3, z.HD, z.F), BF16), reduce_buf,
        dma((z.Q, z.B)), dma((z.Q, z.B)), dma((z.B,)), dma((2, z.B)), dma((z.Q, z.B)), dma((z.Q, z.B)),
        dma((z.Q, z.LV)), dma((z.Q, z.LV)), dma((z.Q, z.LV)), dma((z.Q, z.LV)),
        dma((z.Q, z.LV)), dma((z.Q, z.LV)),
        dma((z.ND,)), dma((z.ND,)), dma((z.ND,)), dma((z.ND,)),
        dma((halves,)), dma((halves,)), dma((1,)), dma((z.B * z.Q,)), dma((halves,)), dma((1,)),
    ]
    grad_state, grads = pl.pallas_call(
        functools.partial(kernel, z),
        out_shape=[
            jax.ShapeDtypeStruct((z.ROWS, z.N), F32),
            jax.ShapeDtypeStruct((z.ND, 3, z.HD, z.F), BF16),
        ],
        in_specs=[any_space] * 4 + [smem] * 2 + [vmem] * 7,
        out_specs=[any_space, any_space],
        scratch_shapes=scratch,
        compiler_params=pltpu.CompilerParams(
            has_side_effects=True, vmem_limit_bytes=60 * 1024 * 1024),
    )(
        checkpoints.reshape(z.S, z.ROWS, z.N),
        final_cot.reshape(z.ROWS, z.N),
        obs_cot.reshape(z.NO, z.F, z.J, z.O),
        legendre,
        obs_time, wave_order, damp, tab_t, tab_w,
        w_in_p.T, w_in_p, w_out_p,
        jnp.broadcast_to(bias[:, None], (z.H, z.O)),
    )
    grads = jnp.swapaxes(grads, 0, 1).astype(F32).reshape(3, z.H, z.F)
    return (
        grad_state.reshape(final_cot.shape),
        from_wire(grads[0].T, 0),
        from_wire(grads[1], 1),
        jnp.sum(grads[2], axis=1),
    )


def solution(mesh):
    placed = (
        P(None, None, "lev", None, "band", None),
        P(None, "lev", None, "band", None),
        P(None, None, None, "band", "lev"),
        P(),
        P(),
        P("band", None, None),
        P(),
        P(),
        P(),
    )
    return jax.shard_map(
        shards,
        mesh=mesh,
        in_specs=placed,
        out_specs=(P(None, "lev", None, "band", None), P(), P(), P()),
        check_vma=False,
    )
```

```python
import functools

import jax
import jax.numpy as jnp
from jax import lax
from jax.experimental import pallas as pl
from jax.experimental.pallas import tpu as pltpu
from jax.sharding import PartitionSpec as P

dt_scale = 1.0
F32 = jnp.float32
BF16 = jnp.bfloat16
MESH = pl.DeviceIdType.MESH
LANES = 128


def dot(a, b):
    return jnp.dot(a, b, preferred_element_type=F32)


def dot_nt(a, b):
    return lax.dot_general(a, b, (((1,), (1,)), ((), ())), preferred_element_type=F32)


class Sizes:
    def __init__(self, bands, levs, steps, fields, levels, waves, wave_count, lat, lon, nobs, hidden):
        self.B, self.LV, self.S, self.NO = bands, levs, steps, nobs
        self.V, self.L, self.R, self.N = fields, levels, waves, wave_count
        self.J, self.O, self.H = lat, lon, hidden
        self.RP = waves // 2
        self.RT = self.RP * bands
        self.JJ = min(16, lat)
        self.Q = lat // self.JJ
        self.VL = fields * levels
        self.C = 4 * self.VL
        self.F = self.VL * levs
        self.ND = bands * levs
        self.HD = hidden // self.ND
        self.PITCH = self.JJ + 8
        self.OPITCH = self.F + 8
        self.ROWS = self.VL * 2 * waves
        self.G = min(8, self.JJ)
        self.HC = min(256, hidden)
        self.joint = lat % (8 * levs) == 0 and self.RP % 4 == 0
        if self.joint:
            self.JD, self.JQ, self.RG = lat // levs, 4, 4
            self.Q = self.JD // self.JQ


def kernel(
    z, ck, fc, obs, leg, obs_time, wave, w_in_raw, w_out_raw, bias_raw,
    out, gout,
    tab_t, tab_w, w_in_t, w_in, w_out, bias, orders, damp,
    tab, adj, tsend, trecv, fsend, frecv, bsend, brecv,
    lf_send, lf_recv, lt_send, lt_recv, lg_send, lg_recv,
    fs, fs2, cstage, ostage, obs_all, obs_s, acc_in, acc_out, acc_b,
    rs_send, rs_recv, ag_send, ag_recv,
    t_s, t_r, f_s, f_r, b_s, b_r, lf_s, lf_r, lt_s, lt_r, lg_s, lg_r, rs_s, rs_r, ag_s, ag_r,
    ck_sem, fc_sem, obs_sem, leg_sem, out_sem, g_sem,
):
    me_b = lax.axis_index("band")
    me_l = lax.axis_index("lev")
    me = me_b * z.LV + me_l

    def to_band(src, dst, ssem, rsem, b):
        return pltpu.make_async_remote_copy(
            src_ref=src, dst_ref=dst, send_sem=ssem, recv_sem=rsem,
            device_id=(b, me_l), device_id_type=MESH,
        )

    def to_lev(src, dst, ssem, rsem, v):
        return pltpu.make_async_remote_copy(
            src_ref=src, dst_ref=dst, send_sem=ssem, recv_sem=rsem,
            device_id=(me_b, v), device_id_type=MESH,
        )

    def others(count, own, body):
        def step(d, _):
            off = d + 1
            body(lax.rem(own + off, count))
            return 0

        lax.fori_loop(0, count - 1, step, 0)

    def band_send(send, recv, ssem, rsem, q):
        others(z.B, me_b, lambda b: to_band(
            send.at[b, q], recv.at[me_b, q], ssem.at[q, b], rsem.at[q, me_b], b).start())
        recv[me_b, q] = send[me_b, q]

    def band_wait_recv(send, recv, ssem, rsem, q):
        others(z.B, me_b, lambda b: to_band(
            send.at[b, q], recv.at[b, q], ssem.at[q, b], rsem.at[q, b], b).wait_recv())

    def band_wait_send(send, recv, ssem, rsem, q):
        others(z.B, me_b, lambda b: to_band(
            send.at[b, q], recv.at[b, q], ssem.at[q, b], rsem.at[q, b], b).wait_send())

    def feat_send(par, q):
        others(z.B, me_b, lambda b: to_band(
            fsend.at[b, q], frecv.at[par, me_b, q], f_s.at[q, b], f_r.at[par, q, me_b], b).start())
        frecv[par, me_b, q] = fsend[me_b, q]

    def feat_wait_recv(par, q):
        others(z.B, me_b, lambda b: to_band(
            fsend.at[b, q], frecv.at[par, b, q], f_s.at[q, b], f_r.at[par, q, b], b).wait_recv())

    def feat_wait_send():
        for q in range(z.Q):
            others(z.B, me_b, lambda b: to_band(
                fsend.at[b, q], frecv.at[0, b, q], f_s.at[q, b], f_r.at[0, q, b], b).wait_send())

    def lev_send(send, recv, ssem, rsem, q):
        others(z.LV, me_l, lambda v: to_lev(
            send.at[v, q], recv.at[me_l, q], ssem.at[q, v], rsem.at[q, me_l], v).start())
        recv[me_l, q] = send[me_l, q]

    def lev_wait_recv(send, recv, ssem, rsem, q):
        others(z.LV, me_l, lambda v: to_lev(
            send.at[v, q], recv.at[v, q], ssem.at[q, v], rsem.at[q, v], v).wait_recv())

    def lev_wait_send(send, recv, ssem, rsem, q):
        others(z.LV, me_l, lambda v: to_lev(
            send.at[v, q], recv.at[v, q], ssem.at[q, v], rsem.at[q, v], v).wait_send())

    def ck_copy(k, h):
        return pltpu.make_async_copy(
            ck.at[k, :, pl.ds(h * LANES, LANES)], cstage.at[h], ck_sem.at[h])

    def fc_copy(h):
        return pltpu.make_async_copy(
            fc.at[:, pl.ds(h * LANES, LANES)], ostage.at[h], fc_sem.at[h])

    halves = z.N // LANES
    bj = z.B * z.JJ
    if z.Q == 1:
        leg_copies = [pltpu.make_async_copy(leg, tab.at[:, 0], leg_sem.at[0])]
    else:
        leg_copies = [
            pltpu.make_async_copy(
                leg.at[:, pl.ds(b * z.J + q * z.JJ, z.JJ), :],
                tab.at[:, q, pl.ds(b * z.JJ, z.JJ), :],
                leg_sem.at[b * z.Q + q],
            )
            for b in range(z.B)
            for q in range(z.Q)
        ]
    obs_copy = pltpu.make_async_copy(obs, obs_all, obs_sem.at[0])
    for h in range(halves):
        ck_copy(z.S - 1, h).start()
    for c in leg_copies:
        c.start()
    for h in range(halves):
        fc_copy(h).start()
    obs_copy.start()

    half_c = 2 * z.VL
    degree = lax.broadcasted_iota(jnp.int32, (half_c, z.N), 1)

    def upper(rp, r2):
        return degree >= wave[me_b * z.R + 2 * rp + r2]

    def rows_of(stage, rp):
        parts = []
        for r2 in range(2):
            for p in range(2):
                start = p * z.R + 2 * rp + r2
                parts.append(jnp.concatenate(
                    [stage[h, pl.ds(start, z.VL, stride=2 * z.R), :] for h in range(halves)], axis=1))
        return jnp.concatenate(parts, axis=0)

    lane = lax.broadcasted_iota(jnp.int32, (z.Q * bj, z.C), 1)

    def legendre(s, rp, send):
        masked = jnp.concatenate(
            [jnp.where(upper(rp, r2), s[r2 * half_c:(r2 + 1) * half_c], 0.0) for r2 in range(2)],
            axis=0).astype(BF16)
        sums = [dot_nt(tab[2 * rp + r2].reshape(z.Q * bj, z.N), masked) for r2 in range(2)]
        sums = jnp.where(lane < half_c, sums[0], sums[1])
        for q in range(z.Q):
            for b in range(z.B):
                row = q * bj + b * z.JJ
                send[b, q, rp] = sums[row:row + z.JJ].astype(BF16)

    def features_legendre():
        def body(rp, _):
            legendre(rows_of(cstage, rp), rp, fsend)
            return 0

        lax.fori_loop(0, z.RP, body, 0, unroll=2)

    def tangent_legendre():
        def body(rp, _):
            damped = damp[...] * adj[rp]
            adj[rp] = damped
            legendre(dt_scale * damped, rp, tsend)
            return 0

        lax.fori_loop(0, z.RP, body, 0, unroll=2)

    def fourier(recv, q, table, scale, send):
        def convert(b, _):
            block = recv[b, q].astype(F32)
            for rp in range(z.RP):
                row = pl.multiple_of((b * z.RP + rp) * z.PITCH, 8)
                fs[pl.ds(row, z.JJ), :] = block[rp]
            return 0

        lax.fori_loop(0, z.B, convert, 0)

        def group(g, _):
            parts = []
            for i in range(z.G):
                at = fs[pl.ds(g * z.G + i, z.RT, stride=z.PITCH), :].T.astype(BF16)
                parts.append(jnp.concatenate(
                    [at[c * z.VL:(c + 1) * z.VL] for c in range(4)], axis=1))
            y = dot(jnp.concatenate(parts, axis=0), table[...])
            if scale is not None:
                y = y * scale
            y = y.astype(BF16)
            for v in range(z.LV):
                for i in range(z.G):
                    send[v, q, g * z.G + i] = y[i * z.VL:(i + 1) * z.VL, v * z.O:(v + 1) * z.O]
            return 0

        lax.fori_loop(0, z.JJ // z.G, group, 0)

    def adjoint_fourier(q):
        def group(g, _):
            x = jnp.concatenate([
                jnp.concatenate([lg_recv[v, q, g * z.G + i] for v in range(z.LV)], axis=1)
                for i in range(z.G)], axis=0)
            y = dot_nt(x, tab_w[...])
            for i in range(z.G):
                yi = y[i * z.VL:(i + 1) * z.VL]
                st = jnp.concatenate([yi[:, c * z.RT:(c + 1) * z.RT] for c in range(4)], axis=0)
                fs2[pl.ds(g * z.G + i, z.RT, stride=z.PITCH), :] = st.T
            return 0

        lax.fori_loop(0, z.JJ // z.G, group, 0)

        def convert(b, _):
            for rp in range(z.RP):
                row = pl.multiple_of((b * z.RP + rp) * z.PITCH, 8)
                bsend[b, q, rp] = fs2[pl.ds(row, z.JJ), :].astype(BF16)
            return 0

        lax.fori_loop(0, z.B, convert, 0)

    def adjoint_legendre(q):
        def body(rp, _):
            b_t = jnp.concatenate(
                [brecv[b, q, rp].astype(F32) for b in range(z.B)], axis=0).T.astype(BF16)
            for r2 in range(2):
                rows = slice(r2 * half_c, (r2 + 1) * half_c)
                grad = dot(b_t[rows], tab[2 * rp + r2, q])
                adj[rp, rows] = adj[rp, rows] + jnp.where(upper(rp, r2), grad, 0.0)
            return 0

        lax.fori_loop(0, z.RP, body, 0, unroll=2)

    def observations(k):
        weights = [jnp.where(obs_time[i] == k, 1.0, 0.0).astype(F32) for i in range(z.NO)]

        def body(f, _):
            v, rest = f // z.LV // z.L, lax.rem(f, z.LV * z.L)
            row = (rest // z.L) * z.VL + v * z.L + lax.rem(rest, z.L)
            total = weights[0] * obs_all[0, f]
            for i in range(1, z.NO):
                total = total + weights[i] * obs_all[i, f]
            obs_s[pl.ds(row, z.J, stride=z.OPITCH), :] = total
            return 0

        lax.fori_loop(0, z.F, body, 0, unroll=4)

    ng = min(4, z.JJ)

    def network(q):
        def group(g, _):
            def columns(ref):
                return jnp.concatenate([
                    jnp.concatenate([ref[v, q, g * ng + i] for v in range(z.LV)], axis=0)
                    for i in range(ng)], axis=1)

            x = columns(lf_recv)
            t = columns(lt_recv)
            grad = None
            for h in range(0, z.H, z.HC):
                rows = slice(h, h + z.HC)
                b = bias[rows]
                pre = dot(w_in_t[rows], x) + jnp.concatenate([b] * ng, axis=1)
                logistic = 0.5 * jnp.tanh(0.5 * pre) + 0.5
                hid = pre * logistic
                pg = dot(w_out[rows], t) * (logistic + hid * (1.0 - logistic))
                low = pg.astype(BF16)
                acc_out[rows] += dot_nt(hid.astype(BF16), t)
                acc_in[rows] += dot_nt(low, x)
                total = pg[:, :z.O]
                for i in range(1, ng):
                    total = total + pg[:, i * z.O:(i + 1) * z.O]
                acc_b[rows] += total
                part = dot(w_in[:, rows], low)
                grad = part if grad is None else grad + part
            for i in range(ng):
                j = q * z.JJ + g * ng + i
                row = pl.multiple_of(j * z.OPITCH, 8)
                col = grad[:, i * z.O:(i + 1) * z.O] + obs_s[pl.ds(row, z.F), :]
                col = col.astype(BF16)
                for v in range(z.LV):
                    lg_send[v, q, g * ng + i] = col[v * z.VL:(v + 1) * z.VL]
            return 0

        lax.fori_loop(0, z.JJ // ng, group, 0)

    def prepare():
        def wire(w):
            return jnp.concatenate([
                w[(v * z.LV + l) * z.L:(v * z.LV + l + 1) * z.L]
                for l in range(z.LV) for v in range(z.V)], axis=0)

        wi = wire(w_in_raw[...].astype(F32))
        w_in[...] = wi.astype(BF16)
        w_in_t[...] = wi.T.astype(BF16)
        w_out[...] = wire(w_out_raw[...].astype(F32).T).T.astype(BF16)
        bias[...] = jnp.broadcast_to(bias_raw[...], (z.O, z.H)).T

        def fill(i, _):
            for r2 in range(2):
                orders[pl.ds(r2 * z.RT + i, 1), :] = jnp.full((1, LANES), wave[2 * i + r2], jnp.int32)
            return 0

        lax.fori_loop(0, z.RT, fill, 0, unroll=4)
        lon = z.O * z.LV
        for r2 in range(2):
            order = orders[r2 * z.RT:(r2 + 1) * z.RT]
            weight = jnp.where(order == 0, 1.0, 2.0).astype(F32)
            for tile in range(lon // LANES):
                cols = slice(tile * LANES, (tile + 1) * LANES)
                longitude = lax.broadcasted_iota(jnp.int32, (z.RT, LANES), 1) + tile * LANES
                turn = (order * longitude).astype(F32)
                turn = turn - jnp.floor(turn * (1.0 / lon)) * lon
                angle = (2.0 * jnp.pi / lon) * turn
                for p, value in enumerate((jnp.cos(angle), -jnp.sin(angle))):
                    rows = slice((2 * r2 + p) * z.RT, (2 * r2 + p + 1) * z.RT)
                    value = value.astype(BF16)
                    tab_t[rows, cols] = value
                    tab_w[rows, cols] = (value.astype(F32) * weight).astype(BF16)

    def to_device(src, dst, ssem, rsem, d):
        return pltpu.make_async_remote_copy(
            src_ref=src, dst_ref=dst, send_sem=ssem, recv_sem=rsem,
            device_id=(d // z.LV, lax.rem(d, z.LV)), device_id_type=MESH,
        )

    def reduce_send():
        for i, acc in enumerate((acc_in, acc_out, acc_b)):
            for d in range(z.ND):
                rs_send[d, i] = acc[d * z.HD:(d + 1) * z.HD].astype(BF16)
        rs_recv[me] = rs_send[me]
        others(z.ND, me, lambda d: to_device(
            rs_send.at[d], rs_recv.at[me], rs_s.at[d], rs_r.at[me], d).start())

    def gather_send():
        others(z.ND, me, lambda d: to_device(
            rs_send.at[d], rs_recv.at[d], rs_s.at[d], rs_r.at[d], d).wait())
        total = rs_recv[0].astype(F32)
        for d in range(1, z.ND):
            total = total + rs_recv[d].astype(F32)
        total = total.astype(BF16)
        ag_send[...] = total
        ag_recv[me] = total
        others(z.ND, me, lambda d: to_device(
            ag_send, ag_recv.at[me], ag_s.at[d], ag_r.at[me], d).start())

    def gather_wait():
        others(z.ND, me, lambda d: to_device(
            ag_send, ag_recv.at[d], ag_s.at[d], ag_r.at[d], d).wait())

    for h in range(halves):
        ck_copy(z.S - 1, h).wait()
    for c in leg_copies:
        c.wait()
    features_legendre()
    feat_send((z.S - 1) % 2, 0)
    if z.S > 1:
        for h in range(halves):
            ck_copy(z.S - 2, h).start()
    degrees = lax.broadcasted_iota(jnp.int32, (1, z.N), 1).astype(F32)
    damp[...] = 1.0 / (1.0 + 2.0 * degrees * (degrees + 1.0) / (z.N * z.N))
    for h in range(halves):
        fc_copy(h).wait()

    def initial(rp, _):
        adj[rp] = rows_of(ostage, rp)
        return 0

    lax.fori_loop(0, z.RP, initial, 0)

    tang = (tsend, trecv, t_s, t_r)
    back = (bsend, brecv, b_s, b_r)
    lt = (lt_send, lt_recv, lt_s, lt_r)
    lf = (lf_send, lf_recv, lf_s, lf_r)
    lg = (lg_send, lg_recv, lg_s, lg_r)

    tangent_legendre()
    for q in range(z.Q):
        if q > 0:
            feat_send((z.S - 1) % 2, q)
        band_send(*tang, q)
    acc_in[...] = jnp.zeros_like(acc_in)
    acc_out[...] = jnp.zeros_like(acc_out)
    acc_b[...] = jnp.zeros_like(acc_b)
    prepare()
    obs_copy.wait()

    def step(i, _):
        k = z.S - 1 - i
        par = lax.rem(k, 2)

        def do_f(q):
            feat_wait_recv(par, q)
            fourier(frecv.at[par], q, tab_w, None, lf_send)
            lev_send(*lf, q)

        def do_t(q):
            band_wait_recv(*tang, q)
            fourier(trecv, q, tab_t, 1.0 / (z.O * z.LV), lt_send)
            lev_send(*lt, q)

        def do_n(q):
            lev_wait_recv(*lf, q)
            lev_wait_recv(*lt, q)
            network(q)
            lev_send(*lg, q)

        def do_b(q):
            lev_wait_recv(*lg, q)

            @pl.when(i > 0)
            def _():
                band_wait_send(*back, q)

            adjoint_fourier(q)
            band_send(*back, q)

        do_f(0)

        @pl.when(k > 0)
        def _():
            for h in range(halves):
                ck_copy(k - 1, h).wait()
            feat_wait_send()
            features_legendre()
            feat_send(1 - par, 0)

        @pl.when(k > 1)
        def _():
            for h in range(halves):
                ck_copy(k - 2, h).start()

        observations(k)
        do_t(0)
        for q in range(1, z.Q):
            do_f(q)
        do_n(0)
        for q in range(1, z.Q):
            do_t(q)
            do_b(q - 1)
            do_n(q)

        @pl.when(k == 0)
        def _():
            reduce_send()

        do_b(z.Q - 1)

        @pl.when(k > 0)
        def _():
            for q in range(1, z.Q):
                feat_send(1 - par, q)

        @pl.when(k == 0)
        def _():
            gather_send()

        for q in range(z.Q):
            band_wait_recv(*back, q)
            adjoint_legendre(q)
        for q in range(z.Q):
            band_wait_send(*tang, q)

        @pl.when(k > 0)
        def _():
            tangent_legendre()
            for q in range(z.Q):
                band_send(*tang, q)

        for q in range(z.Q):
            lev_wait_send(*lf, q)
            lev_wait_send(*lt, q)
            lev_wait_send(*lg, q)
        return 0

    lax.fori_loop(0, z.S, step, 0)
    adj_copy = pltpu.make_async_copy(adj, out, out_sem.at[0])
    adj_copy.start()
    gather_wait()
    gather_copy = pltpu.make_async_copy(ag_recv, gout, g_sem.at[0])
    gather_copy.start()
    feat_wait_send()
    for q in range(z.Q):
        band_wait_send(*back, q)
    adj_copy.wait()
    gather_copy.wait()


def joint_kernel(
    z, ck, fc, obs, leg, obs_time, wave, w_in_raw, w_out_raw, bias_raw,
    out, gout,
    tab_t, tab_w, w_in_t, w_in, w_out, bias, orders, damp,
    tab, adj, tsend, trecv, fsend, frecv, bsend, brecv, osend, orecv,
    feats, tangs, fs, fs2, cstage, ostage, obs_all, obs_s, acc_in, acc_out, acc_b,
    rs_send, rs_recv, ag_send, ag_recv,
    t_s, t_r, f_s, f_r, b_s, b_r, o_s, o_r, rs_s, rs_r, ag_s, ag_r,
    ck_sem, fc_sem, obs_sem, leg_sem, out_sem, g_sem,
):
    me_b = lax.axis_index("band")
    me_l = lax.axis_index("lev")
    me = me_b * z.LV + me_l
    halves = z.N // LANES
    lon = z.O * z.LV
    half_c = 2 * z.VL

    def others(count, own, body):
        def step(d, _):
            body(lax.rem(own + d, count))
            return 0

        lax.fori_loop(1, count, step, 0)

    def remote(src, dst, ssem, rsem, d):
        return pltpu.make_async_remote_copy(
            src_ref=src, dst_ref=dst, send_sem=ssem, recv_sem=rsem,
            device_id=(d // z.LV, lax.rem(d, z.LV)), device_id_type=MESH,
        )

    def send_all(send, recv, ssem, rsem, q):
        others(z.ND, me, lambda d: remote(
            send.at[d, q], recv.at[me, q], ssem.at[q, d], rsem.at[q, me], d).start())
        recv[me, q] = send[me, q]

    def wait_recv(send, recv, ssem, rsem, q):
        others(z.ND, me, lambda d: remote(
            send.at[d, q], recv.at[d, q], ssem.at[q, d], rsem.at[q, d], d).wait_recv())

    def wait_send(send, recv, ssem, rsem, q):
        others(z.ND, me, lambda d: remote(
            send.at[d, q], recv.at[d, q], ssem.at[q, d], rsem.at[q, d], d).wait_send())

    def obs_send(par):
        others(z.LV, me_l, lambda v: remote(
            osend.at[v], orecv.at[par, me_l], o_s.at[v], o_r.at[par, me_l],
            me_b * z.LV + v).start())
        orecv[par, me_l] = osend[me_l]

    def obs_wait_recv(par):
        others(z.LV, me_l, lambda v: remote(
            osend.at[v], orecv.at[par, v], o_s.at[v], o_r.at[par, v],
            me_b * z.LV + v).wait_recv())

    def obs_wait_send():
        others(z.LV, me_l, lambda v: remote(
            osend.at[v], orecv.at[0, v], o_s.at[v], o_r.at[0, v],
            me_b * z.LV + v).wait_send())

    def ck_copy(k, h):
        return pltpu.make_async_copy(
            ck.at[k, :, pl.ds(h * LANES, LANES)], cstage.at[h], ck_sem.at[h])

    def fc_copy(h):
        return pltpu.make_async_copy(
            fc.at[:, pl.ds(h * LANES, LANES)], ostage.at[h], fc_sem.at[h])

    leg_copy = pltpu.make_async_copy(leg, tab, leg_sem.at[0])
    obs_copy = pltpu.make_async_copy(obs, obs_all, obs_sem.at[0])
    for h in range(halves):
        ck_copy(z.S - 1, h).start()
    leg_copy.start()
    for h in range(halves):
        fc_copy(h).start()
    obs_copy.start()

    degree = lax.broadcasted_iota(jnp.int32, (half_c, z.N), 1)

    def upper(rp, r2):
        return degree >= wave[me_b * z.R + 2 * rp + r2]

    def rows_of(stage, rp):
        parts = []
        for r2 in range(2):
            for p in range(2):
                start = p * z.R + 2 * rp + r2
                parts.append(jnp.concatenate(
                    [stage[h, pl.ds(start, z.VL, stride=2 * z.R), :] for h in range(halves)], axis=1))
        return jnp.concatenate(parts, axis=0)

    lat = z.ND * z.JD
    lane = lax.broadcasted_iota(jnp.int32, (lat, z.C), 1)

    def legendre(s, rp):
        masked = jnp.concatenate(
            [jnp.where(upper(rp, r2), s[r2 * half_c:(r2 + 1) * half_c], 0.0) for r2 in range(2)],
            axis=0).astype(BF16)
        sums = [dot_nt(tab[2 * rp + r2], masked) for r2 in range(2)]
        return jnp.where(lane < half_c, sums[0], sums[1]).reshape(z.ND, z.JD, z.C)

    def legendre_groups(spectral, send):
        def body(g, _):
            sums = [legendre(spectral(g * z.RG + i), g * z.RG + i) for i in range(z.RG)]
            row = pl.multiple_of(g * z.RG * z.JQ, z.RG * z.JQ)
            for q in range(z.Q):
                block = jnp.concatenate(
                    [s[:, q * z.JQ:(q + 1) * z.JQ] for s in sums], axis=1)
                send[:, q, pl.ds(row, z.RG * z.JQ), :] = block.astype(BF16)
            return 0

        lax.fori_loop(0, z.RP // z.RG, body, 0)

    def features_legendre():
        legendre_groups(lambda rp: rows_of(cstage, rp), fsend)

    def tangent_legendre():
        def damped(rp):
            value = damp[...] * adj[rp]
            adj[rp] = value
            return dt_scale * value

        legendre_groups(damped, tsend)

    block = z.RP * z.JQ

    def fourier(recv, q, table, scale, dst):
        def convert(b, _):
            for v in range(z.LV):
                row = pl.multiple_of((v * z.B + b) * block, block)
                fs[pl.ds(row, block), :] = recv[b * z.LV + v, q].astype(F32)
            return 0

        lax.fori_loop(0, z.B, convert, 0, unroll=2)
        parts = []
        for i in range(z.JQ):
            for v in range(z.LV):
                at = fs[pl.ds(v * z.B * block + i, z.RT, stride=z.JQ), :].T.astype(BF16)
                parts.append(jnp.concatenate(
                    [at[c * z.VL:(c + 1) * z.VL] for c in range(4)], axis=1))
        y = dot(jnp.concatenate(parts, axis=0), table[...])
        if scale is not None:
            y = y * scale
        y = y.astype(BF16)
        for i in range(z.JQ):
            dst[q * z.JQ + i] = y[i * z.F:(i + 1) * z.F]

    def network(q, par):
        def column(i, _):
            j = q * z.JQ + i
            x = feats[j]
            t = tangs[j]
            grad = None
            for h in range(0, z.H, z.HC):
                rows = slice(h, h + z.HC)
                pre = dot(w_in_t[rows], x) + jnp.concatenate([bias[rows]] * z.LV, axis=1)
                logistic = 0.5 * jnp.tanh(0.5 * pre) + 0.5
                hid = pre * logistic
                pg = dot(w_out[rows], t) * (logistic + hid * (1.0 - logistic))
                low = pg.astype(BF16)
                acc_out[rows] += dot_nt(hid.astype(BF16), t)
                acc_in[rows] += dot_nt(low, x)
                total = pg[:, :z.O]
                for v in range(1, z.LV):
                    total = total + pg[:, v * z.O:(v + 1) * z.O]
                acc_b[rows] += total
                part = dot(w_in[:, rows], low)
                grad = part if grad is None else grad + part
            grad = grad + jnp.concatenate(
                [orecv[par, v, j].astype(F32) for v in range(z.LV)], axis=1)
            y = dot_nt(grad.astype(BF16), tab_w[...])
            for v in range(z.LV):
                yv = y[v * z.VL:(v + 1) * z.VL]
                st = jnp.concatenate([yv[:, c * z.RT:(c + 1) * z.RT] for c in range(4)], axis=0)
                fs2[pl.ds(v * z.B * block + i, z.RT, stride=z.JQ), :] = st.T
            return 0

        lax.fori_loop(0, z.JQ, column, 0)

        def convert(b, _):
            for v in range(z.LV):
                row = pl.multiple_of((v * z.B + b) * block, block)
                bsend[b * z.LV + v, q] = fs2[pl.ds(row, block), :].astype(BF16)
            return 0

        lax.fori_loop(0, z.B, convert, 0, unroll=2)

    def adjoint_legendre():
        def body(g, _):
            row = pl.multiple_of(g * z.RG * z.JQ, z.RG * z.JQ)
            chunks = [brecv[:, q, pl.ds(row, z.RG * z.JQ), :].astype(F32) for q in range(z.Q)]
            for i in range(z.RG):
                rp = g * z.RG + i
                b_t = jnp.concatenate(
                    [c[:, i * z.JQ:(i + 1) * z.JQ] for c in chunks],
                    axis=1).reshape(lat, z.C).T.astype(BF16)
                for r2 in range(2):
                    rows = slice(r2 * half_c, (r2 + 1) * half_c)
                    grad = dot(b_t[rows], tab[2 * rp + r2])
                    adj[rp, rows] = adj[rp, rows] + jnp.where(upper(rp, r2), grad, 0.0)
            return 0

        lax.fori_loop(0, z.RP // z.RG, body, 0)

    def observations(k):
        weights = [jnp.where(obs_time[i] == k, 1.0, 0.0).astype(F32) for i in range(z.NO)]

        def body(f, _):
            v, rest = f // z.LV // z.L, lax.rem(f, z.LV * z.L)
            row = (rest // z.L) * z.VL + v * z.L + lax.rem(rest, z.L)
            total = weights[0] * obs_all[0, f]
            for i in range(1, z.NO):
                total = total + weights[i] * obs_all[i, f]
            obs_s[pl.ds(row, z.J, stride=z.OPITCH), :] = total
            return 0

        lax.fori_loop(0, z.F, body, 0, unroll=4)

        def pack(v, _):
            for j in range(z.JD):
                row = pl.multiple_of((v * z.JD + j) * z.OPITCH, 8)
                osend[v, j] = obs_s[pl.ds(row, z.F), :].astype(BF16)
            return 0

        lax.fori_loop(0, z.LV, pack, 0)

    def prepare():
        def wire(w):
            return jnp.concatenate([
                w[(v * z.LV + l) * z.L:(v * z.LV + l + 1) * z.L]
                for l in range(z.LV) for v in range(z.V)], axis=0)

        wi = wire(w_in_raw[...].astype(F32))
        w_in[...] = wi.astype(BF16)
        w_in_t[...] = wi.T.astype(BF16)
        w_out[...] = wire(w_out_raw[...].astype(F32).T).T.astype(BF16)
        bias[...] = jnp.broadcast_to(bias_raw[...], (z.O, z.H)).T

        def fill(i, _):
            for r2 in range(2):
                orders[pl.ds(r2 * z.RT + i, 1), :] = jnp.full((1, LANES), wave[2 * i + r2], jnp.int32)
            return 0

        lax.fori_loop(0, z.RT, fill, 0, unroll=4)
        for r2 in range(2):
            order = orders[r2 * z.RT:(r2 + 1) * z.RT]
            weight = jnp.where(order == 0, 1.0, 2.0).astype(F32)
            for tile in range(lon // LANES):
                cols = slice(tile * LANES, (tile + 1) * LANES)
                longitude = lax.broadcasted_iota(jnp.int32, (z.RT, LANES), 1) + tile * LANES
                turn = (order * longitude).astype(F32)
                turn = turn - jnp.floor(turn * (1.0 / lon)) * lon
                angle = (2.0 * jnp.pi / lon) * turn
                for p, value in enumerate((jnp.cos(angle), -jnp.sin(angle))):
                    rows = slice((2 * r2 + p) * z.RT, (2 * r2 + p + 1) * z.RT)
                    value = value.astype(BF16)
                    tab_t[rows, cols] = value
                    tab_w[rows, cols] = (value.astype(F32) * weight).astype(BF16)

    def reduce_send():
        for i, acc in enumerate((acc_in, acc_out, acc_b)):
            for d in range(z.ND):
                rs_send[d, i] = acc[d * z.HD:(d + 1) * z.HD].astype(BF16)
        rs_recv[me] = rs_send[me]
        others(z.ND, me, lambda d: remote(
            rs_send.at[d], rs_recv.at[me], rs_s.at[d], rs_r.at[me], d).start())

    def gather_send():
        others(z.ND, me, lambda d: remote(
            rs_send.at[d], rs_recv.at[d], rs_s.at[d], rs_r.at[d], d).wait())
        total = rs_recv[0].astype(F32)
        for d in range(1, z.ND):
            total = total + rs_recv[d].astype(F32)
        total = total.astype(BF16)
        ag_send[...] = total
        ag_recv[me] = total
        others(z.ND, me, lambda d: remote(
            ag_send, ag_recv.at[me], ag_s.at[d], ag_r.at[me], d).start())

    def gather_wait():
        others(z.ND, me, lambda d: remote(
            ag_send, ag_recv.at[d], ag_s.at[d], ag_r.at[d], d).wait())

    for h in range(halves):
        ck_copy(z.S - 1, h).wait()
    leg_copy.wait()
    tang = (tsend, trecv, t_s, t_r)
    back = (bsend, brecv, b_s, b_r)

    def feat(par):
        return (fsend, frecv.at[par], f_s, f_r.at[par])

    features_legendre()
    first = (z.S - 1) % 2
    send_all(*feat(first), 0)
    if z.S > 1:
        for h in range(halves):
            ck_copy(z.S - 2, h).start()
    degrees = lax.broadcasted_iota(jnp.int32, (1, z.N), 1).astype(F32)
    damp[...] = 1.0 / (1.0 + 2.0 * degrees * (degrees + 1.0) / (z.N * z.N))
    for h in range(halves):
        fc_copy(h).wait()

    def initial(rp, _):
        adj[rp] = rows_of(ostage, rp)
        return 0

    lax.fori_loop(0, z.RP, initial, 0)
    tangent_legendre()
    for q in range(z.Q):
        if q > 0:
            send_all(*feat(first), q)
        send_all(*tang, q)
    obs_copy.wait()
    observations(z.S - 1)
    obs_send(first)
    acc_in[...] = jnp.zeros_like(acc_in)
    acc_out[...] = jnp.zeros_like(acc_out)
    acc_b[...] = jnp.zeros_like(acc_b)
    prepare()

    def step(i, _):
        k = z.S - 1 - i
        par = lax.rem(k, 2)

        def do_f(q):
            wait_recv(*feat(par), q)
            fourier(frecv.at[par], q, tab_w, None, feats)

        def do_n(q):
            wait_recv(*tang, q)
            fourier(trecv, q, tab_t, 1.0 / lon, tangs)
            if q == 0:
                obs_wait_recv(par)

            @pl.when(i > 0)
            def _():
                wait_send(*back, q)

            network(q, par)
            send_all(*back, q)

        do_f(0)

        @pl.when(k > 0)
        def _():
            for h in range(halves):
                ck_copy(k - 1, h).wait()
            for q in range(z.Q):
                wait_send(*feat(0), q)
            features_legendre()
            send_all(*feat(1 - par), 0)

        @pl.when(k > 1)
        def _():
            for h in range(halves):
                ck_copy(k - 2, h).start()

        do_n(0)

        @pl.when(k > 0)
        def _():
            obs_wait_send()
            observations(k - 1)
            obs_send(1 - par)

        for q in range(1, z.Q):
            do_f(q)
            do_n(q)

        @pl.when(k == 0)
        def _():
            reduce_send()

        @pl.when(k > 0)
        def _():
            for q in range(1, z.Q):
                send_all(*feat(1 - par), q)

        @pl.when(k == 0)
        def _():
            gather_send()

        for q in range(z.Q):
            wait_recv(*back, q)
        adjoint_legendre()
        for q in range(z.Q):
            wait_send(*tang, q)

        @pl.when(k > 0)
        def _():
            tangent_legendre()
            for q in range(z.Q):
                send_all(*tang, q)

        return 0

    lax.fori_loop(0, z.S, step, 0)
    adj_copy = pltpu.make_async_copy(adj, out, out_sem.at[0])
    adj_copy.start()
    gather_wait()
    gather_copy = pltpu.make_async_copy(ag_recv, gout, g_sem.at[0])
    gather_copy.start()
    obs_wait_send()
    for q in range(z.Q):
        wait_send(*feat(0), q)
        wait_send(*back, q)
    adj_copy.wait()
    gather_copy.wait()


def finish(z, adj, grads, out, grad_in, grad_out, grad_bias, stage, flat, sem):
    half_c = 2 * z.VL
    copies = []
    for h in range(z.N // LANES):
        cols = slice(h * LANES, (h + 1) * LANES)

        def body(rp, _):
            for r2 in range(2):
                for p in range(2):
                    start = p * z.R + 2 * rp + r2
                    c = r2 * half_c + p * z.VL
                    stage[h, pl.ds(start, z.VL, stride=2 * z.R), :] = adj[rp, c:c + z.VL, cols]
            return 0

        lax.fori_loop(0, z.RP, body, 0)
        copy = pltpu.make_async_copy(stage.at[h], out.at[:, pl.ds(h * LANES, LANES)], sem.at[h])
        copy.start()
        copies.append(copy)

    for d in range(z.ND):
        for i in range(3):
            flat[i, d * z.HD:(d + 1) * z.HD] = grads[d, i].astype(F32)

    def from_wire(w):
        return jnp.concatenate([
            w[(l * z.V + v) * z.L:(l * z.V + v + 1) * z.L]
            for v in range(z.V) for l in range(z.LV)], axis=0)

    grad_in[...] = from_wire(flat[0].T)
    grad_out[...] = from_wire(flat[1].T).T
    grad_bias[...] = jnp.sum(flat[2].T, axis=0, keepdims=True)
    for copy in copies:
        copy.wait()


def shards(checkpoints, final_cot, obs_cot, obs_time, wave_order, legendre, w_in, w_out, bias):
    local_waves, lat_count, wave_count = legendre.shape
    fields, levels = final_cot.shape[:2]
    z = Sizes(
        lax.axis_size("band"), lax.axis_size("lev"), checkpoints.shape[0], fields, levels,
        local_waves, wave_count, obs_cot.shape[3], obs_cot.shape[4], obs_cot.shape[0],
        w_in.shape[1])
    any_space = pl.BlockSpec(memory_space=pl.ANY)
    smem = pl.BlockSpec(memory_space=pltpu.SMEM)
    vmem = pl.BlockSpec(memory_space=pltpu.VMEM)
    dma = pltpu.SemaphoreType.DMA
    halves = z.N // LANES
    reduce_buf = pltpu.VMEM((z.ND, 3, z.HD, z.F), BF16)
    lon = z.O * z.LV
    weights = [
        pltpu.VMEM((4 * z.RT, lon), BF16), pltpu.VMEM((4 * z.RT, lon), BF16),
        pltpu.VMEM((z.H, z.F), BF16), pltpu.VMEM((z.F, z.H), BF16), pltpu.VMEM((z.H, z.F), BF16),
        pltpu.VMEM((z.H, z.O), F32), pltpu.VMEM((2 * z.RT, LANES), jnp.int32), pltpu.VMEM((1, z.N), F32),
    ]
    stages = [
        pltpu.VMEM((halves, z.ROWS, LANES), F32),
        pltpu.VMEM((halves, z.ROWS, LANES), F32),
        pltpu.VMEM((z.NO, z.F, z.J, z.O), F32),
        pltpu.VMEM((z.J * z.OPITCH, z.O), F32),
        pltpu.VMEM((z.H, z.F), F32), pltpu.VMEM((z.H, z.F), F32), pltpu.VMEM((z.H, z.O), F32),
        reduce_buf, reduce_buf,
        pltpu.VMEM((3, z.HD, z.F), BF16), reduce_buf,
    ]
    reduce_sems = [dma((z.ND,))] * 4
    if z.joint:
        body = joint_kernel
        block = (z.ND, z.Q, z.RP * z.JQ, z.C)
        buf = pltpu.VMEM(block, BF16)
        obs_buf = (z.LV, z.JD, z.F, z.O)
        flat = pltpu.VMEM((z.ND * z.RP * z.JQ, z.C), F32)
        columns = pltpu.VMEM((z.JD, z.F, lon), BF16)
        pair = dma((z.Q, z.ND))
        scratch = weights + [
            pltpu.VMEM((z.R, z.ND * z.JD, z.N), BF16),
            pltpu.VMEM((z.RP, z.C, z.N), F32),
            buf, buf, buf, pltpu.VMEM((2,) + block, BF16), buf, buf,
            pltpu.VMEM(obs_buf, BF16), pltpu.VMEM((2,) + obs_buf, BF16),
            columns, columns, flat, flat,
        ] + stages + [
            pair, pair, pair, dma((2, z.Q, z.ND)), pair, pair,
            dma((z.LV,)), dma((2, z.LV)),
        ] + reduce_sems + [
            dma((halves,)), dma((halves,)), dma((1,)), dma((1,)), dma((1,)), dma((1,)),
        ]
    else:
        body = kernel
        band_buf = pltpu.VMEM((z.B, z.Q, z.RP, z.JJ, z.C), BF16)
        lev_buf = pltpu.VMEM((z.LV, z.Q, z.JJ, z.VL, z.O), BF16)
        flat = pltpu.VMEM((z.RT * z.PITCH, z.C), F32)
        scratch = weights + [
            pltpu.VMEM((z.R, z.Q, z.B * z.JJ, z.N), BF16),
            pltpu.VMEM((z.RP, z.C, z.N), F32),
            band_buf, band_buf, band_buf,
            pltpu.VMEM((2, z.B, z.Q, z.RP, z.JJ, z.C), BF16),
            band_buf, band_buf,
            lev_buf, lev_buf, lev_buf, lev_buf, lev_buf, lev_buf,
            flat, flat,
        ] + stages + [
            dma((z.Q, z.B)), dma((z.Q, z.B)), dma((z.Q, z.B)), dma((2, z.Q, z.B)),
            dma((z.Q, z.B)), dma((z.Q, z.B)),
            dma((z.Q, z.LV)), dma((z.Q, z.LV)), dma((z.Q, z.LV)), dma((z.Q, z.LV)),
            dma((z.Q, z.LV)), dma((z.Q, z.LV)),
        ] + reduce_sems + [
            dma((halves,)), dma((halves,)), dma((1,)), dma((z.B * z.Q,)), dma((1,)), dma((1,)),
        ]
    state, grads = pl.pallas_call(
        functools.partial(body, z),
        out_shape=[
            jax.ShapeDtypeStruct((z.RP, z.C, z.N), F32),
            jax.ShapeDtypeStruct((z.ND, 3, z.HD, z.F), BF16),
        ],
        in_specs=[any_space] * 4 + [smem] * 2 + [vmem] * 3,
        out_specs=[any_space, any_space],
        scratch_shapes=scratch,
        compiler_params=pltpu.CompilerParams(
            has_side_effects=True, vmem_limit_bytes=60 * 1024 * 1024),
    )(
        checkpoints.reshape(z.S, z.ROWS, z.N),
        final_cot.reshape(z.ROWS, z.N),
        obs_cot.reshape(z.NO, z.F, z.J, z.O),
        legendre,
        obs_time, wave_order, w_in, w_out, bias[None],
    )
    grad_state, grad_in, grad_out, grad_bias = pl.pallas_call(
        functools.partial(finish, z),
        out_shape=[
            jax.ShapeDtypeStruct((z.ROWS, z.N), F32),
            jax.ShapeDtypeStruct((z.F, z.H), F32),
            jax.ShapeDtypeStruct((z.H, z.F), F32),
            jax.ShapeDtypeStruct((1, z.H), F32),
        ],
        in_specs=[vmem, vmem],
        out_specs=[any_space, vmem, vmem, vmem],
        scratch_shapes=[
            pltpu.VMEM((halves, z.ROWS, LANES), F32),
            pltpu.VMEM((3, z.H, z.F), F32),
            dma((halves,)),
        ],
        compiler_params=pltpu.CompilerParams(vmem_limit_bytes=40 * 1024 * 1024),
    )(state, grads)
    return grad_state.reshape(final_cot.shape), grad_in, grad_out, grad_bias[0]


def solution(mesh):
    placed = (
        P(None, None, "lev", None, "band", None),
        P(None, "lev", None, "band", None),
        P(None, None, None, "band", "lev"),
        P(),
        P(),
        P("band", None, None),
        P(),
        P(),
        P(),
    )
    return jax.shard_map(
        shards,
        mesh=mesh,
        in_specs=placed,
        out_specs=(P(None, "lev", None, "band", None), P(), P(), P()),
        check_vma=False,
    )
```

```python
import functools

import jax
import jax.numpy as jnp
from jax import lax
from jax.experimental import pallas as pl
from jax.experimental.pallas import tpu as pltpu
from jax.sharding import PartitionSpec as P

dt_scale = 1.0
F32 = jnp.float32
BF16 = jnp.bfloat16
MESH = pl.DeviceIdType.MESH
LANES = 128


def dot(a, b):
    return jnp.dot(a, b, preferred_element_type=F32)


def dot_nt(a, b):
    return lax.dot_general(a, b, (((1,), (1,)), ((), ())), preferred_element_type=F32)


class Sizes:
    def __init__(self, bands, levs, steps, fields, levels, waves, wave_count, lat, lon, nobs, hidden):
        self.B, self.LV, self.S, self.NO = bands, levs, steps, nobs
        self.V, self.L, self.R, self.N = fields, levels, waves, wave_count
        self.J, self.O, self.H = lat, lon, hidden
        self.RP = waves // 2
        self.RT = self.RP * bands
        self.PR = 2 * waves + 8
        self.JJ = min(16, lat)
        self.Q = lat // self.JJ
        self.VL = fields * levels
        self.C = 4 * self.VL
        self.F = self.VL * levs
        self.ND = bands * levs
        self.HD = hidden // self.ND
        self.PITCH = self.JJ + 8
        self.OPITCH = self.F + 8
        self.ROWS = self.VL * 2 * waves
        self.G = min(8, self.JJ)
        self.HC = min(256, hidden)
        self.joint = lat % (8 * levs) == 0 and self.RP % 4 == 0
        if self.joint:
            self.JD, self.JQ, self.RG = lat // levs, 4, 4
            self.Q = self.JD // self.JQ


def kernel(
    z, ck, fc, obs, leg, obs_time, wave, w_in_raw, w_out_raw, bias_raw,
    out, gout,
    tab_t, tab_w, w_in_t, w_in, w_out, bias, orders, damp,
    tab, adj, tsend, trecv, fsend, frecv, bsend, brecv,
    lf_send, lf_recv, lt_send, lt_recv, lg_send, lg_recv,
    fs, fs2, cstage, ostage, obs_all, obs_s, acc_in, acc_out, acc_b,
    rs_send, rs_recv, ag_send, ag_recv,
    t_s, t_r, f_s, f_r, b_s, b_r, lf_s, lf_r, lt_s, lt_r, lg_s, lg_r, rs_s, rs_r, ag_s, ag_r,
    ck_sem, fc_sem, obs_sem, leg_sem, out_sem, g_sem,
):
    me_b = lax.axis_index("band")
    me_l = lax.axis_index("lev")
    me = me_b * z.LV + me_l

    def to_band(src, dst, ssem, rsem, b):
        return pltpu.make_async_remote_copy(
            src_ref=src, dst_ref=dst, send_sem=ssem, recv_sem=rsem,
            device_id=(b, me_l), device_id_type=MESH,
        )

    def to_lev(src, dst, ssem, rsem, v):
        return pltpu.make_async_remote_copy(
            src_ref=src, dst_ref=dst, send_sem=ssem, recv_sem=rsem,
            device_id=(me_b, v), device_id_type=MESH,
        )

    def others(count, own, body):
        def step(d, _):
            off = d + 1
            body(lax.rem(own + off, count))
            return 0

        lax.fori_loop(0, count - 1, step, 0)

    def band_send(send, recv, ssem, rsem, q):
        others(z.B, me_b, lambda b: to_band(
            send.at[b, q], recv.at[me_b, q], ssem.at[q, b], rsem.at[q, me_b], b).start())
        recv[me_b, q] = send[me_b, q]

    def band_wait_recv(send, recv, ssem, rsem, q):
        others(z.B, me_b, lambda b: to_band(
            send.at[b, q], recv.at[b, q], ssem.at[q, b], rsem.at[q, b], b).wait_recv())

    def band_wait_send(send, recv, ssem, rsem, q):
        others(z.B, me_b, lambda b: to_band(
            send.at[b, q], recv.at[b, q], ssem.at[q, b], rsem.at[q, b], b).wait_send())

    def feat_send(par, q):
        others(z.B, me_b, lambda b: to_band(
            fsend.at[b, q], frecv.at[par, me_b, q], f_s.at[q, b], f_r.at[par, q, me_b], b).start())
        frecv[par, me_b, q] = fsend[me_b, q]

    def feat_wait_recv(par, q):
        others(z.B, me_b, lambda b: to_band(
            fsend.at[b, q], frecv.at[par, b, q], f_s.at[q, b], f_r.at[par, q, b], b).wait_recv())

    def feat_wait_send():
        for q in range(z.Q):
            others(z.B, me_b, lambda b: to_band(
                fsend.at[b, q], frecv.at[0, b, q], f_s.at[q, b], f_r.at[0, q, b], b).wait_send())

    def lev_send(send, recv, ssem, rsem, q):
        others(z.LV, me_l, lambda v: to_lev(
            send.at[v, q], recv.at[me_l, q], ssem.at[q, v], rsem.at[q, me_l], v).start())
        recv[me_l, q] = send[me_l, q]

    def lev_wait_recv(send, recv, ssem, rsem, q):
        others(z.LV, me_l, lambda v: to_lev(
            send.at[v, q], recv.at[v, q], ssem.at[q, v], rsem.at[q, v], v).wait_recv())

    def lev_wait_send(send, recv, ssem, rsem, q):
        others(z.LV, me_l, lambda v: to_lev(
            send.at[v, q], recv.at[v, q], ssem.at[q, v], rsem.at[q, v], v).wait_send())

    def ck_copy(k, h):
        return pltpu.make_async_copy(
            ck.at[k, :, pl.ds(h * LANES, LANES)], cstage.at[h], ck_sem.at[h])

    def fc_copy(h):
        return pltpu.make_async_copy(
            fc.at[:, pl.ds(h * LANES, LANES)], ostage.at[h], fc_sem.at[h])

    halves = z.N // LANES
    bj = z.B * z.JJ
    if z.Q == 1:
        leg_copies = [pltpu.make_async_copy(leg, tab.at[:, 0], leg_sem.at[0])]
    else:
        leg_copies = [
            pltpu.make_async_copy(
                leg.at[:, pl.ds(b * z.J + q * z.JJ, z.JJ), :],
                tab.at[:, q, pl.ds(b * z.JJ, z.JJ), :],
                leg_sem.at[b * z.Q + q],
            )
            for b in range(z.B)
            for q in range(z.Q)
        ]
    obs_copy = pltpu.make_async_copy(obs, obs_all, obs_sem.at[0])
    for h in range(halves):
        ck_copy(z.S - 1, h).start()
    for c in leg_copies:
        c.start()
    for h in range(halves):
        fc_copy(h).start()
    obs_copy.start()

    half_c = 2 * z.VL
    degree = lax.broadcasted_iota(jnp.int32, (half_c, z.N), 1)

    def upper(rp, r2):
        return degree >= wave[me_b * z.R + 2 * rp + r2]

    def rows_of(stage, rp):
        parts = []
        for r2 in range(2):
            for p in range(2):
                start = p * z.R + 2 * rp + r2
                parts.append(jnp.concatenate(
                    [stage[h, pl.ds(start, z.VL, stride=2 * z.R), :] for h in range(halves)], axis=1))
        return jnp.concatenate(parts, axis=0)

    lane = lax.broadcasted_iota(jnp.int32, (z.Q * bj, z.C), 1)

    def legendre(s, rp, send):
        masked = jnp.concatenate(
            [jnp.where(upper(rp, r2), s[r2 * half_c:(r2 + 1) * half_c], 0.0) for r2 in range(2)],
            axis=0).astype(BF16)
        sums = [dot_nt(tab[2 * rp + r2].reshape(z.Q * bj, z.N), masked) for r2 in range(2)]
        sums = jnp.where(lane < half_c, sums[0], sums[1])
        for q in range(z.Q):
            for b in range(z.B):
                row = q * bj + b * z.JJ
                send[b, q, rp] = sums[row:row + z.JJ].astype(BF16)

    def features_legendre():
        def body(rp, _):
            legendre(rows_of(cstage, rp), rp, fsend)
            return 0

        lax.fori_loop(0, z.RP, body, 0, unroll=2)

    def tangent_legendre():
        def body(rp, _):
            damped = damp[...] * adj[rp]
            adj[rp] = damped
            legendre(dt_scale * damped, rp, tsend)
            return 0

        lax.fori_loop(0, z.RP, body, 0, unroll=2)

    def fourier(recv, q, table, scale, send):
        def convert(b, _):
            block = recv[b, q].astype(F32)
            for rp in range(z.RP):
                row = pl.multiple_of((b * z.RP + rp) * z.PITCH, 8)
                fs[pl.ds(row, z.JJ), :] = block[rp]
            return 0

        lax.fori_loop(0, z.B, convert, 0)

        def group(g, _):
            parts = []
            for i in range(z.G):
                at = fs[pl.ds(g * z.G + i, z.RT, stride=z.PITCH), :].T.astype(BF16)
                parts.append(jnp.concatenate(
                    [at[c * z.VL:(c + 1) * z.VL] for c in range(4)], axis=1))
            y = dot(jnp.concatenate(parts, axis=0), table[...])
            if scale is not None:
                y = y * scale
            y = y.astype(BF16)
            for v in range(z.LV):
                for i in range(z.G):
                    send[v, q, g * z.G + i] = y[i * z.VL:(i + 1) * z.VL, v * z.O:(v + 1) * z.O]
            return 0

        lax.fori_loop(0, z.JJ // z.G, group, 0)

    def adjoint_fourier(q):
        def group(g, _):
            x = jnp.concatenate([
                jnp.concatenate([lg_recv[v, q, g * z.G + i] for v in range(z.LV)], axis=1)
                for i in range(z.G)], axis=0)
            y = dot_nt(x, tab_w[...])
            for i in range(z.G):
                yi = y[i * z.VL:(i + 1) * z.VL]
                st = jnp.concatenate([yi[:, c * z.RT:(c + 1) * z.RT] for c in range(4)], axis=0)
                fs2[pl.ds(g * z.G + i, z.RT, stride=z.PITCH), :] = st.T
            return 0

        lax.fori_loop(0, z.JJ // z.G, group, 0)

        def convert(b, _):
            for rp in range(z.RP):
                row = pl.multiple_of((b * z.RP + rp) * z.PITCH, 8)
                bsend[b, q, rp] = fs2[pl.ds(row, z.JJ), :].astype(BF16)
            return 0

        lax.fori_loop(0, z.B, convert, 0)

    def adjoint_legendre(q):
        def body(rp, _):
            b_t = jnp.concatenate(
                [brecv[b, q, rp].astype(F32) for b in range(z.B)], axis=0).T.astype(BF16)
            for r2 in range(2):
                rows = slice(r2 * half_c, (r2 + 1) * half_c)
                grad = dot(b_t[rows], tab[2 * rp + r2, q])
                adj[rp, rows] = adj[rp, rows] + jnp.where(upper(rp, r2), grad, 0.0)
            return 0

        lax.fori_loop(0, z.RP, body, 0, unroll=2)

    def observations(k):
        weights = [jnp.where(obs_time[i] == k, 1.0, 0.0).astype(F32) for i in range(z.NO)]

        def body(f, _):
            v, rest = f // z.LV // z.L, lax.rem(f, z.LV * z.L)
            row = (rest // z.L) * z.VL + v * z.L + lax.rem(rest, z.L)
            total = weights[0] * obs_all[0, f]
            for i in range(1, z.NO):
                total = total + weights[i] * obs_all[i, f]
            obs_s[pl.ds(row, z.J, stride=z.OPITCH), :] = total
            return 0

        lax.fori_loop(0, z.F, body, 0, unroll=4)

    ng = min(4, z.JJ)

    def network(q):
        def group(g, _):
            def columns(ref):
                return jnp.concatenate([
                    jnp.concatenate([ref[v, q, g * ng + i] for v in range(z.LV)], axis=0)
                    for i in range(ng)], axis=1)

            x = columns(lf_recv)
            t = columns(lt_recv)
            grad = None
            for h in range(0, z.H, z.HC):
                rows = slice(h, h + z.HC)
                b = bias[rows]
                pre = dot(w_in_t[rows], x) + jnp.concatenate([b] * ng, axis=1)
                logistic = 0.5 * jnp.tanh(0.5 * pre) + 0.5
                hid = pre * logistic
                pg = dot(w_out[rows], t) * (logistic + hid * (1.0 - logistic))
                low = pg.astype(BF16)
                acc_out[rows] += dot_nt(hid.astype(BF16), t)
                acc_in[rows] += dot_nt(low, x)
                total = pg[:, :z.O]
                for i in range(1, ng):
                    total = total + pg[:, i * z.O:(i + 1) * z.O]
                acc_b[rows] += total
                part = dot(w_in[:, rows], low)
                grad = part if grad is None else grad + part
            for i in range(ng):
                j = q * z.JJ + g * ng + i
                row = pl.multiple_of(j * z.OPITCH, 8)
                col = grad[:, i * z.O:(i + 1) * z.O] + obs_s[pl.ds(row, z.F), :]
                col = col.astype(BF16)
                for v in range(z.LV):
                    lg_send[v, q, g * ng + i] = col[v * z.VL:(v + 1) * z.VL]
            return 0

        lax.fori_loop(0, z.JJ // ng, group, 0)

    def prepare():
        def wire(w):
            return jnp.concatenate([
                w[(v * z.LV + l) * z.L:(v * z.LV + l + 1) * z.L]
                for l in range(z.LV) for v in range(z.V)], axis=0)

        wi = wire(w_in_raw[...].astype(F32))
        w_in[...] = wi.astype(BF16)
        w_in_t[...] = wi.T.astype(BF16)
        w_out[...] = wire(w_out_raw[...].astype(F32).T).T.astype(BF16)
        bias[...] = jnp.broadcast_to(bias_raw[...], (z.O, z.H)).T

        def fill(i, _):
            for r2 in range(2):
                orders[pl.ds(r2 * z.RT + i, 1), :] = jnp.full((1, LANES), wave[2 * i + r2], jnp.int32)
            return 0

        lax.fori_loop(0, z.RT, fill, 0, unroll=4)
        lon = z.O * z.LV
        for r2 in range(2):
            order = orders[r2 * z.RT:(r2 + 1) * z.RT]
            weight = jnp.where(order == 0, 1.0, 2.0).astype(F32)
            for tile in range(lon // LANES):
                cols = slice(tile * LANES, (tile + 1) * LANES)
                longitude = lax.broadcasted_iota(jnp.int32, (z.RT, LANES), 1) + tile * LANES
                turn = (order * longitude).astype(F32)
                turn = turn - jnp.floor(turn * (1.0 / lon)) * lon
                angle = (2.0 * jnp.pi / lon) * turn
                for p, value in enumerate((jnp.cos(angle), -jnp.sin(angle))):
                    rows = slice((2 * r2 + p) * z.RT, (2 * r2 + p + 1) * z.RT)
                    value = value.astype(BF16)
                    tab_t[rows, cols] = value
                    tab_w[rows, cols] = (value.astype(F32) * weight).astype(BF16)

    def to_device(src, dst, ssem, rsem, d):
        return pltpu.make_async_remote_copy(
            src_ref=src, dst_ref=dst, send_sem=ssem, recv_sem=rsem,
            device_id=(d // z.LV, lax.rem(d, z.LV)), device_id_type=MESH,
        )

    def reduce_send():
        for i, acc in enumerate((acc_in, acc_out, acc_b)):
            for d in range(z.ND):
                rs_send[d, i] = acc[d * z.HD:(d + 1) * z.HD].astype(BF16)
        rs_recv[me] = rs_send[me]
        others(z.ND, me, lambda d: to_device(
            rs_send.at[d], rs_recv.at[me], rs_s.at[d], rs_r.at[me], d).start())

    def gather_send():
        others(z.ND, me, lambda d: to_device(
            rs_send.at[d], rs_recv.at[d], rs_s.at[d], rs_r.at[d], d).wait())
        total = rs_recv[0].astype(F32)
        for d in range(1, z.ND):
            total = total + rs_recv[d].astype(F32)
        total = total.astype(BF16)
        ag_send[...] = total
        ag_recv[me] = total
        others(z.ND, me, lambda d: to_device(
            ag_send, ag_recv.at[me], ag_s.at[d], ag_r.at[me], d).start())

    def gather_wait():
        others(z.ND, me, lambda d: to_device(
            ag_send, ag_recv.at[d], ag_s.at[d], ag_r.at[d], d).wait())

    for h in range(halves):
        ck_copy(z.S - 1, h).wait()
    for c in leg_copies:
        c.wait()
    features_legendre()
    feat_send((z.S - 1) % 2, 0)
    if z.S > 1:
        for h in range(halves):
            ck_copy(z.S - 2, h).start()
    degrees = lax.broadcasted_iota(jnp.int32, (1, z.N), 1).astype(F32)
    damp[...] = 1.0 / (1.0 + 2.0 * degrees * (degrees + 1.0) / (z.N * z.N))
    for h in range(halves):
        fc_copy(h).wait()

    def initial(rp, _):
        adj[rp] = rows_of(ostage, rp)
        return 0

    lax.fori_loop(0, z.RP, initial, 0)

    tang = (tsend, trecv, t_s, t_r)
    back = (bsend, brecv, b_s, b_r)
    lt = (lt_send, lt_recv, lt_s, lt_r)
    lf = (lf_send, lf_recv, lf_s, lf_r)
    lg = (lg_send, lg_recv, lg_s, lg_r)

    tangent_legendre()
    for q in range(z.Q):
        if q > 0:
            feat_send((z.S - 1) % 2, q)
        band_send(*tang, q)
    acc_in[...] = jnp.zeros_like(acc_in)
    acc_out[...] = jnp.zeros_like(acc_out)
    acc_b[...] = jnp.zeros_like(acc_b)
    prepare()
    obs_copy.wait()

    def step(i, _):
        k = z.S - 1 - i
        par = lax.rem(k, 2)

        def do_f(q):
            feat_wait_recv(par, q)
            fourier(frecv.at[par], q, tab_w, None, lf_send)
            lev_send(*lf, q)

        def do_t(q):
            band_wait_recv(*tang, q)
            fourier(trecv, q, tab_t, 1.0 / (z.O * z.LV), lt_send)
            lev_send(*lt, q)

        def do_n(q):
            lev_wait_recv(*lf, q)
            lev_wait_recv(*lt, q)
            network(q)
            lev_send(*lg, q)

        def do_b(q):
            lev_wait_recv(*lg, q)

            @pl.when(i > 0)
            def _():
                band_wait_send(*back, q)

            adjoint_fourier(q)
            band_send(*back, q)

        do_f(0)

        @pl.when(k > 0)
        def _():
            for h in range(halves):
                ck_copy(k - 1, h).wait()
            feat_wait_send()
            features_legendre()
            feat_send(1 - par, 0)

        @pl.when(k > 1)
        def _():
            for h in range(halves):
                ck_copy(k - 2, h).start()

        observations(k)
        do_t(0)
        for q in range(1, z.Q):
            do_f(q)
        do_n(0)
        for q in range(1, z.Q):
            do_t(q)
            do_b(q - 1)
            do_n(q)

        @pl.when(k == 0)
        def _():
            reduce_send()

        do_b(z.Q - 1)

        @pl.when(k > 0)
        def _():
            for q in range(1, z.Q):
                feat_send(1 - par, q)

        @pl.when(k == 0)
        def _():
            gather_send()

        for q in range(z.Q):
            band_wait_recv(*back, q)
            adjoint_legendre(q)
        for q in range(z.Q):
            band_wait_send(*tang, q)

        @pl.when(k > 0)
        def _():
            tangent_legendre()
            for q in range(z.Q):
                band_send(*tang, q)

        for q in range(z.Q):
            lev_wait_send(*lf, q)
            lev_wait_send(*lt, q)
            lev_wait_send(*lg, q)
        return 0

    lax.fori_loop(0, z.S, step, 0)
    adj_copy = pltpu.make_async_copy(adj, out, out_sem.at[0])
    adj_copy.start()
    gather_wait()
    gather_copy = pltpu.make_async_copy(ag_recv, gout, g_sem.at[0])
    gather_copy.start()
    feat_wait_send()
    for q in range(z.Q):
        band_wait_send(*back, q)
    adj_copy.wait()
    gather_copy.wait()


def joint_kernel(
    z, ck, fc, obs, leg, obs_time, wave, w_in_raw, w_out_raw, bias_raw,
    out, gout,
    tab_t, tab_w, w_in_t, w_in, w_out, bias, orders, damp,
    tab, adj, tsend, trecv, fsend, frecv, bsend, brecv, osend, orecv,
    feats, tangs, fs, fs2, cstage, ostage, obs_all, obs_s, acc_in, acc_out, acc_b,
    rs_send, rs_recv, rb_send, rb_recv, ag_send, gb_recv, ag_recv,
    t_s, t_r, f_s, f_r, b_s, b_r, o_s, o_r, rl_s, rl_r, rb_s, rb_r,
    ck_sem, fc_sem, obs_sem, leg_sem, out_sem, g_sem,
):
    me_b = lax.axis_index("band")
    me_l = lax.axis_index("lev")
    me = me_b * z.LV + me_l
    halves = z.N // LANES
    lon = z.O * z.LV
    half_c = 2 * z.VL

    def others(count, own, body):
        def step(d, _):
            body(lax.rem(own + d, count))
            return 0

        lax.fori_loop(1, count, step, 0)

    def remote(src, dst, ssem, rsem, d):
        return pltpu.make_async_remote_copy(
            src_ref=src, dst_ref=dst, send_sem=ssem, recv_sem=rsem,
            device_id=(d // z.LV, lax.rem(d, z.LV)), device_id_type=MESH,
        )

    def send_all(send, recv, ssem, rsem, q):
        others(z.ND, me, lambda d: remote(
            send.at[d, q], recv.at[me, q], ssem.at[q, d], rsem.at[q, me], d).start())
        recv[me, q] = send[me, q]

    def wait_recv(send, recv, ssem, rsem, q):
        others(z.ND, me, lambda d: remote(
            send.at[d, q], recv.at[d, q], ssem.at[q, d], rsem.at[q, d], d).wait_recv())

    def wait_send(send, recv, ssem, rsem, q):
        others(z.ND, me, lambda d: remote(
            send.at[d, q], recv.at[d, q], ssem.at[q, d], rsem.at[q, d], d).wait_send())

    def obs_send(par):
        others(z.LV, me_l, lambda v: remote(
            osend.at[v], orecv.at[par, me_l], o_s.at[v], o_r.at[par, me_l],
            me_b * z.LV + v).start())
        orecv[par, me_l] = osend[me_l]

    def obs_wait_recv(par):
        others(z.LV, me_l, lambda v: remote(
            osend.at[v], orecv.at[par, v], o_s.at[v], o_r.at[par, v],
            me_b * z.LV + v).wait_recv())

    def obs_wait_send():
        others(z.LV, me_l, lambda v: remote(
            osend.at[v], orecv.at[0, v], o_s.at[v], o_r.at[0, v],
            me_b * z.LV + v).wait_send())

    def stage_copies(src, stage, sem, h):
        def copy(v, _):
            pltpu.make_async_copy(
                src.at[pl.ds(v * 2 * z.R, 2 * z.R), pl.ds(h * LANES, LANES)],
                stage.at[h, pl.ds(v * z.PR, 2 * z.R)], sem.at[h]).start()
            return 0

        lax.fori_loop(0, z.VL, copy, 0)

    def stage_wait(src, stage, sem, h):
        pltpu.make_async_copy(
            src.at[:, pl.ds(h * LANES, LANES)], stage.at[h, pl.ds(0, z.ROWS)], sem.at[h]).wait()

    leg_copy = pltpu.make_async_copy(leg, tab, leg_sem.at[0])
    obs_copy = pltpu.make_async_copy(obs, obs_all, obs_sem.at[0])
    for h in range(halves):
        stage_copies(ck.at[z.S - 1], cstage, ck_sem, h)
    leg_copy.start()
    for h in range(halves):
        stage_copies(fc, ostage, fc_sem, h)
    obs_copy.start()

    degree = lax.broadcasted_iota(jnp.int32, (half_c, z.N), 1)

    def upper(rp, r2):
        return degree >= wave[me_b * z.R + 2 * rp + r2]

    def rows_of(stage, rp):
        parts = []
        for r2 in range(2):
            for p in range(2):
                start = p * z.R + 2 * rp + r2
                parts.append(jnp.concatenate(
                    [stage[h, pl.ds(start, z.VL, stride=z.PR), :] for h in range(halves)], axis=1))
        return jnp.concatenate(parts, axis=0)

    lat = z.ND * z.JD
    lane = lax.broadcasted_iota(jnp.int32, (lat, z.C), 1)

    def legendre(s, rp):
        masked = jnp.concatenate(
            [jnp.where(upper(rp, r2), s[r2 * half_c:(r2 + 1) * half_c], 0.0) for r2 in range(2)],
            axis=0).astype(BF16)
        sums = [dot_nt(tab[2 * rp + r2], masked) for r2 in range(2)]
        return jnp.where(lane < half_c, sums[0], sums[1]).reshape(z.ND, z.JD, z.C)

    def legendre_groups(spectral, send):
        def body(g, _):
            sums = [legendre(spectral(g * z.RG + i), g * z.RG + i) for i in range(z.RG)]
            row = pl.multiple_of(g * z.RG * z.JQ, z.RG * z.JQ)
            for q in range(z.Q):
                block = jnp.concatenate(
                    [s[:, q * z.JQ:(q + 1) * z.JQ] for s in sums], axis=1)
                send[:, q, pl.ds(row, z.RG * z.JQ), :] = block.astype(BF16)
            return 0

        lax.fori_loop(0, z.RP // z.RG, body, 0)

    def features_legendre():
        legendre_groups(lambda rp: rows_of(cstage, rp), fsend)

    def tangent_legendre():
        def damped(rp):
            value = damp[...] * adj[rp]
            adj[rp] = value
            return dt_scale * value

        legendre_groups(damped, tsend)

    block = z.RP * z.JQ

    def fourier(recv, q, table, scale, dst):
        def convert(b, _):
            for v in range(z.LV):
                row = pl.multiple_of((v * z.B + b) * block, block)
                fs[pl.ds(row, block), :] = recv[b * z.LV + v, q].astype(F32)
            return 0

        lax.fori_loop(0, z.B, convert, 0, unroll=2)
        parts = []
        for i in range(z.JQ):
            for v in range(z.LV):
                at = fs[pl.ds(v * z.B * block + i, z.RT, stride=z.JQ), :].T.astype(BF16)
                parts.append(jnp.concatenate(
                    [at[c * z.VL:(c + 1) * z.VL] for c in range(4)], axis=1))
        y = dot(jnp.concatenate(parts, axis=0), table[...])
        if scale is not None:
            y = y * scale
        y = y.astype(BF16)
        for i in range(z.JQ):
            dst[q * z.JQ + i] = y[i * z.F:(i + 1) * z.F]

    def network(q, par):
        def column(i, _):
            j = q * z.JQ + i
            x = feats[j]
            t = tangs[j]
            grad = None
            for h in range(0, z.H, z.HC):
                rows = slice(h, h + z.HC)
                pre = dot(w_in_t[rows], x) + jnp.concatenate([bias[rows]] * z.LV, axis=1)
                logistic = 0.5 * jnp.tanh(0.5 * pre) + 0.5
                hid = pre * logistic
                pg = dot(w_out[rows], t) * (logistic + hid * (1.0 - logistic))
                low = pg.astype(BF16)
                acc_out[rows] += dot_nt(hid.astype(BF16), t)
                acc_in[rows] += dot_nt(low, x)
                total = pg[:, :z.O]
                for v in range(1, z.LV):
                    total = total + pg[:, v * z.O:(v + 1) * z.O]
                acc_b[rows] += total
                part = dot(w_in[:, rows], low)
                grad = part if grad is None else grad + part
            grad = grad + jnp.concatenate(
                [orecv[par, v, j].astype(F32) for v in range(z.LV)], axis=1)
            y = dot_nt(grad.astype(BF16), tab_w[...])
            for v in range(z.LV):
                yv = y[v * z.VL:(v + 1) * z.VL]
                st = jnp.concatenate([yv[:, c * z.RT:(c + 1) * z.RT] for c in range(4)], axis=0)
                fs2[pl.ds(v * z.B * block + i, z.RT, stride=z.JQ), :] = st.T
            return 0

        lax.fori_loop(0, z.JQ, column, 0)

        def convert(b, _):
            for v in range(z.LV):
                row = pl.multiple_of((v * z.B + b) * block, block)
                bsend[b * z.LV + v, q] = fs2[pl.ds(row, block), :].astype(BF16)
            return 0

        lax.fori_loop(0, z.B, convert, 0, unroll=2)

    def adjoint_legendre():
        def body(g, _):
            row = pl.multiple_of(g * z.RG * z.JQ, z.RG * z.JQ)
            chunks = [brecv[:, q, pl.ds(row, z.RG * z.JQ), :].astype(F32) for q in range(z.Q)]
            for i in range(z.RG):
                rp = g * z.RG + i
                b_t = jnp.concatenate(
                    [c[:, i * z.JQ:(i + 1) * z.JQ] for c in chunks],
                    axis=1).reshape(lat, z.C).T.astype(BF16)
                for r2 in range(2):
                    rows = slice(r2 * half_c, (r2 + 1) * half_c)
                    grad = dot(b_t[rows], tab[2 * rp + r2])
                    adj[rp, rows] = adj[rp, rows] + jnp.where(upper(rp, r2), grad, 0.0)
            return 0

        lax.fori_loop(0, z.RP // z.RG, body, 0)

    def observations(k):
        weights = [jnp.where(obs_time[i] == k, 1.0, 0.0).astype(F32) for i in range(z.NO)]

        def body(f, _):
            v, rest = f // z.LV // z.L, lax.rem(f, z.LV * z.L)
            row = (rest // z.L) * z.VL + v * z.L + lax.rem(rest, z.L)
            total = weights[0] * obs_all[0, f]
            for i in range(1, z.NO):
                total = total + weights[i] * obs_all[i, f]
            obs_s[pl.ds(row, z.J, stride=z.OPITCH), :] = total
            return 0

        lax.fori_loop(0, z.F, body, 0, unroll=4)

        def pack(v, _):
            for j in range(z.JD):
                row = pl.multiple_of((v * z.JD + j) * z.OPITCH, 8)
                osend[v, j] = obs_s[pl.ds(row, z.F), :].astype(BF16)
            return 0

        lax.fori_loop(0, z.LV, pack, 0)

    def prepare():
        def wire(w):
            return jnp.concatenate([
                w[(v * z.LV + l) * z.L:(v * z.LV + l + 1) * z.L]
                for l in range(z.LV) for v in range(z.V)], axis=0)

        wi = wire(w_in_raw[...].astype(F32))
        w_in[...] = wi.astype(BF16)
        w_in_t[...] = wi.T.astype(BF16)
        w_out[...] = wire(w_out_raw[...].astype(F32).T).T.astype(BF16)
        bias[...] = jnp.broadcast_to(bias_raw[...], (z.O, z.H)).T

        def fill(i, _):
            for r2 in range(2):
                orders[pl.ds(r2 * z.RT + i, 1), :] = jnp.full((1, LANES), wave[2 * i + r2], jnp.int32)
            return 0

        lax.fori_loop(0, z.RT, fill, 0, unroll=4)
        for r2 in range(2):
            order = orders[r2 * z.RT:(r2 + 1) * z.RT]
            weight = jnp.where(order == 0, 1.0, 2.0).astype(F32)
            for tile in range(lon // LANES):
                cols = slice(tile * LANES, (tile + 1) * LANES)
                longitude = lax.broadcasted_iota(jnp.int32, (z.RT, LANES), 1) + tile * LANES
                turn = (order * longitude).astype(F32)
                turn = turn - jnp.floor(turn * (1.0 / lon)) * lon
                angle = (2.0 * jnp.pi / lon) * turn
                for p, value in enumerate((jnp.cos(angle), -jnp.sin(angle))):
                    rows = slice((2 * r2 + p) * z.RT, (2 * r2 + p + 1) * z.RT)
                    value = value.astype(BF16)
                    tab_t[rows, cols] = value
                    tab_w[rows, cols] = (value.astype(F32) * weight).astype(BF16)

    def lev_copy(src, dst, stage, mine, v):
        return remote(src, dst, rl_s.at[stage, v], rl_r.at[stage, mine], me_b * z.LV + v)

    def band_copy(src, dst, stage, mine, b):
        return remote(src, dst, rb_s.at[stage, b], rb_r.at[stage, mine], b * z.LV + me_l)

    def reduce_lev():
        for i, acc in enumerate((acc_in, acc_out, acc_b)):
            for v in range(z.LV):
                for b in range(z.B):
                    row = (v * z.B + b) * z.HD
                    rs_send[v, b, i] = acc[row:row + z.HD].astype(BF16)
        rs_recv[me_l] = rs_send[me_l]
        others(z.LV, me_l, lambda v: lev_copy(
            rs_send.at[v], rs_recv.at[me_l], 0, me_l, v).start())

    def reduce_band():
        others(z.LV, me_l, lambda v: lev_copy(
            rs_send.at[v], rs_recv.at[v], 0, v, v).wait())

        def add(b, _):
            total = rs_recv[0, b].astype(F32)
            for v in range(1, z.LV):
                total = total + rs_recv[v, b].astype(F32)
            rb_send[b] = total.astype(BF16)
            return 0

        lax.fori_loop(0, z.B, add, 0)
        rb_recv[me_b] = rb_send[me_b]
        others(z.B, me_b, lambda b: band_copy(
            rb_send.at[b], rb_recv.at[me_b], 0, me_b, b).start())

    def gather_band():
        others(z.B, me_b, lambda b: band_copy(
            rb_send.at[b], rb_recv.at[b], 0, b, b).wait())
        total = rb_recv[0].astype(F32)
        for b in range(1, z.B):
            total = total + rb_recv[b].astype(F32)
        total = total.astype(BF16)
        ag_send[...] = total
        gb_recv[me_b] = total
        others(z.B, me_b, lambda b: band_copy(
            ag_send, gb_recv.at[me_b], 1, me_b, b).start())

    def gather_lev():
        others(z.B, me_b, lambda b: band_copy(
            ag_send, gb_recv.at[b], 1, b, b).wait())
        ag_recv[me_l] = gb_recv[...]
        others(z.LV, me_l, lambda v: lev_copy(
            gb_recv, ag_recv.at[me_l], 1, me_l, v).start())

    def gather_wait():
        others(z.LV, me_l, lambda v: lev_copy(
            gb_recv, ag_recv.at[v], 1, v, v).wait())

    for h in range(halves):
        stage_wait(ck.at[z.S - 1], cstage, ck_sem, h)
    leg_copy.wait()
    tang = (tsend, trecv, t_s, t_r)
    back = (bsend, brecv, b_s, b_r)

    def feat(par):
        return (fsend, frecv.at[par], f_s, f_r.at[par])

    features_legendre()
    first = (z.S - 1) % 2
    send_all(*feat(first), 0)
    if z.S > 1:
        for h in range(halves):
            stage_copies(ck.at[z.S - 2], cstage, ck_sem, h)
    degrees = lax.broadcasted_iota(jnp.int32, (1, z.N), 1).astype(F32)
    damp[...] = 1.0 / (1.0 + 2.0 * degrees * (degrees + 1.0) / (z.N * z.N))
    for h in range(halves):
        stage_wait(fc, ostage, fc_sem, h)

    def initial(rp, _):
        adj[rp] = rows_of(ostage, rp)
        return 0

    lax.fori_loop(0, z.RP, initial, 0)
    tangent_legendre()
    for q in range(z.Q):
        if q > 0:
            send_all(*feat(first), q)
        send_all(*tang, q)
    obs_copy.wait()
    observations(z.S - 1)
    obs_send(first)
    acc_in[...] = jnp.zeros_like(acc_in)
    acc_out[...] = jnp.zeros_like(acc_out)
    acc_b[...] = jnp.zeros_like(acc_b)
    prepare()

    def step(i, _):
        k = z.S - 1 - i
        par = lax.rem(k, 2)

        def do_f(q):
            wait_recv(*feat(par), q)
            fourier(frecv.at[par], q, tab_w, None, feats)

        def do_n(q):
            wait_recv(*tang, q)
            fourier(trecv, q, tab_t, 1.0 / lon, tangs)
            if q == 0:
                obs_wait_recv(par)

            @pl.when(i > 0)
            def _():
                wait_send(*back, q)

            network(q, par)
            if q == z.Q - 1:
                @pl.when(k == 0)
                def _():
                    reduce_lev()

            send_all(*back, q)

        do_f(0)

        @pl.when(k > 0)
        def _():
            for h in range(halves):
                stage_wait(ck.at[k - 1], cstage, ck_sem, h)
            for q in range(z.Q):
                wait_send(*feat(0), q)
            features_legendre()
            send_all(*feat(1 - par), 0)

        @pl.when(k > 1)
        def _():
            for h in range(halves):
                stage_copies(ck.at[k - 2], cstage, ck_sem, h)

        do_n(0)

        @pl.when(k > 0)
        def _():
            obs_wait_send()
            observations(k - 1)
            obs_send(1 - par)

        for q in range(1, z.Q):
            do_f(q)
            do_n(q)

        @pl.when(k > 0)
        def _():
            for q in range(1, z.Q):
                send_all(*feat(1 - par), q)

        @pl.when(k == 0)
        def _():
            reduce_band()

        for q in range(z.Q):
            wait_recv(*back, q)

        @pl.when(k == 0)
        def _():
            gather_band()

        adjoint_legendre()
        for q in range(z.Q):
            wait_send(*tang, q)

        @pl.when(k > 0)
        def _():
            tangent_legendre()
            for q in range(z.Q):
                send_all(*tang, q)

        return 0

    lax.fori_loop(0, z.S, step, 0)
    adj_copy = pltpu.make_async_copy(adj, out, out_sem.at[0])
    adj_copy.start()
    gather_lev()
    gather_wait()
    gather_copy = pltpu.make_async_copy(ag_recv, gout, g_sem.at[0])
    gather_copy.start()
    obs_wait_send()
    for q in range(z.Q):
        wait_send(*feat(0), q)
        wait_send(*back, q)
    adj_copy.wait()
    gather_copy.wait()


def finish(z, adj_hbm, grads_hbm, out, grad_in, grad_out, grad_bias, adj, grads, stage, flat, sem, in_sem):
    half_c = 2 * z.VL
    halves = z.N // LANES
    grads_copy = pltpu.make_async_copy(grads_hbm, grads, in_sem.at[halves])
    adj_copies = [
        pltpu.make_async_copy(adj_hbm.at[:, :, pl.ds(h * LANES, LANES)], adj.at[h], in_sem.at[h])
        for h in range(halves)
    ]
    for copy in adj_copies:
        copy.start()
    grads_copy.start()
    for h in range(halves):
        adj_copies[h].wait()

        def body(rp, _):
            for r2 in range(2):
                for p in range(2):
                    start = p * z.R + 2 * rp + r2
                    c = r2 * half_c + p * z.VL
                    stage[h, pl.ds(start, z.VL, stride=z.PR), :] = adj[h, rp, c:c + z.VL]
            return 0

        lax.fori_loop(0, z.RP, body, 0, unroll=2)

        def store(v, _):
            pltpu.make_async_copy(
                stage.at[h, pl.ds(v * z.PR, 2 * z.R)],
                out.at[pl.ds(v * 2 * z.R, 2 * z.R), pl.ds(h * LANES, LANES)], sem.at[h]).start()
            return 0

        lax.fori_loop(0, z.VL, store, 0)

    grads_copy.wait()
    for d in range(z.ND):
        for i in range(3):
            flat[i, d * z.HD:(d + 1) * z.HD] = grads[d, i].astype(F32)

    def from_wire(w):
        return jnp.concatenate([
            w[(l * z.V + v) * z.L:(l * z.V + v + 1) * z.L]
            for v in range(z.V) for l in range(z.LV)], axis=0)

    grad_in[...] = from_wire(flat[0].T)
    grad_out[...] = from_wire(flat[1].T).T
    grad_bias[...] = jnp.sum(flat[2].T, axis=0, keepdims=True)
    for h in range(halves):
        pltpu.make_async_copy(
            stage.at[h, pl.ds(0, z.ROWS)], out.at[:, pl.ds(h * LANES, LANES)], sem.at[h]).wait()


def shards(checkpoints, final_cot, obs_cot, obs_time, wave_order, legendre, w_in, w_out, bias):
    local_waves, lat_count, wave_count = legendre.shape
    fields, levels = final_cot.shape[:2]
    z = Sizes(
        lax.axis_size("band"), lax.axis_size("lev"), checkpoints.shape[0], fields, levels,
        local_waves, wave_count, obs_cot.shape[3], obs_cot.shape[4], obs_cot.shape[0],
        w_in.shape[1])
    any_space = pl.BlockSpec(memory_space=pl.ANY)
    smem = pl.BlockSpec(memory_space=pltpu.SMEM)
    vmem = pl.BlockSpec(memory_space=pltpu.VMEM)
    dma = pltpu.SemaphoreType.DMA
    halves = z.N // LANES
    reduce_buf = pltpu.VMEM((z.ND, 3, z.HD, z.F), BF16)
    lon = z.O * z.LV
    weights = [
        pltpu.VMEM((4 * z.RT, lon), BF16), pltpu.VMEM((4 * z.RT, lon), BF16),
        pltpu.VMEM((z.H, z.F), BF16), pltpu.VMEM((z.F, z.H), BF16), pltpu.VMEM((z.H, z.F), BF16),
        pltpu.VMEM((z.H, z.O), F32), pltpu.VMEM((2 * z.RT, LANES), jnp.int32), pltpu.VMEM((1, z.N), F32),
    ]
    stage_rows = z.VL * z.PR if z.joint else z.ROWS
    stages = [
        pltpu.VMEM((halves, stage_rows, LANES), F32),
        pltpu.VMEM((halves, stage_rows, LANES), F32),
        pltpu.VMEM((z.NO, z.F, z.J, z.O), F32),
        pltpu.VMEM((z.J * z.OPITCH, z.O), F32),
        pltpu.VMEM((z.H, z.F), F32), pltpu.VMEM((z.H, z.F), F32), pltpu.VMEM((z.H, z.O), F32),
    ]
    part = pltpu.VMEM((3, z.HD, z.F), BF16)
    grads_shape = (z.ND, 3, z.HD, z.F)
    if z.joint:
        body = joint_kernel
        grads_shape = (z.LV, z.B, 3, z.HD, z.F)
        reduce_buf = pltpu.VMEM(grads_shape, BF16)
        band_part = pltpu.VMEM(grads_shape[1:], BF16)
        block = (z.ND, z.Q, z.RP * z.JQ, z.C)
        buf = pltpu.VMEM(block, BF16)
        obs_buf = (z.LV, z.JD, z.F, z.O)
        flat = pltpu.VMEM((z.ND * z.RP * z.JQ, z.C), F32)
        columns = pltpu.VMEM((z.JD, z.F, lon), BF16)
        pair = dma((z.Q, z.ND))
        scratch = weights + [
            pltpu.VMEM((z.R, z.ND * z.JD, z.N), BF16),
            pltpu.VMEM((z.RP, z.C, z.N), F32),
            buf, buf, buf, pltpu.VMEM((2,) + block, BF16), buf, buf,
            pltpu.VMEM(obs_buf, BF16), pltpu.VMEM((2,) + obs_buf, BF16),
            columns, columns, flat, flat,
        ] + stages + [
            reduce_buf, reduce_buf, band_part, band_part, part, band_part, reduce_buf,
            pair, pair, pair, dma((2, z.Q, z.ND)), pair, pair,
            dma((z.LV,)), dma((2, z.LV)),
            dma((2, z.LV)), dma((2, z.LV)), dma((2, z.B)), dma((2, z.B)),
            dma((halves,)), dma((halves,)), dma((1,)), dma((1,)), dma((1,)), dma((1,)),
        ]
    else:
        body = kernel
        band_buf = pltpu.VMEM((z.B, z.Q, z.RP, z.JJ, z.C), BF16)
        lev_buf = pltpu.VMEM((z.LV, z.Q, z.JJ, z.VL, z.O), BF16)
        flat = pltpu.VMEM((z.RT * z.PITCH, z.C), F32)
        scratch = weights + [
            pltpu.VMEM((z.R, z.Q, z.B * z.JJ, z.N), BF16),
            pltpu.VMEM((z.RP, z.C, z.N), F32),
            band_buf, band_buf, band_buf,
            pltpu.VMEM((2, z.B, z.Q, z.RP, z.JJ, z.C), BF16),
            band_buf, band_buf,
            lev_buf, lev_buf, lev_buf, lev_buf, lev_buf, lev_buf,
            flat, flat,
        ] + stages + [
            reduce_buf, reduce_buf, part, reduce_buf,
            dma((z.Q, z.B)), dma((z.Q, z.B)), dma((z.Q, z.B)), dma((2, z.Q, z.B)),
            dma((z.Q, z.B)), dma((z.Q, z.B)),
            dma((z.Q, z.LV)), dma((z.Q, z.LV)), dma((z.Q, z.LV)), dma((z.Q, z.LV)),
            dma((z.Q, z.LV)), dma((z.Q, z.LV)),
            dma((z.ND,)), dma((z.ND,)), dma((z.ND,)), dma((z.ND,)),
            dma((halves,)), dma((halves,)), dma((1,)), dma((z.B * z.Q,)), dma((1,)), dma((1,)),
        ]
    state, grads = pl.pallas_call(
        functools.partial(body, z),
        out_shape=[
            jax.ShapeDtypeStruct((z.RP, z.C, z.N), F32),
            jax.ShapeDtypeStruct(grads_shape, BF16),
        ],
        in_specs=[any_space] * 4 + [smem] * 2 + [vmem] * 3,
        out_specs=[any_space, any_space],
        scratch_shapes=scratch,
        compiler_params=pltpu.CompilerParams(
            has_side_effects=True, vmem_limit_bytes=60 * 1024 * 1024),
    )(
        checkpoints.reshape(z.S, z.ROWS, z.N),
        final_cot.reshape(z.ROWS, z.N),
        obs_cot.reshape(z.NO, z.F, z.J, z.O),
        legendre,
        obs_time, wave_order, w_in, w_out, bias[None],
    )
    grad_state, grad_in, grad_out, grad_bias = pl.pallas_call(
        functools.partial(finish, z),
        out_shape=[
            jax.ShapeDtypeStruct((z.ROWS, z.N), F32),
            jax.ShapeDtypeStruct((z.F, z.H), F32),
            jax.ShapeDtypeStruct((z.H, z.F), F32),
            jax.ShapeDtypeStruct((1, z.H), F32),
        ],
        in_specs=[any_space, any_space],
        out_specs=[any_space, vmem, vmem, vmem],
        scratch_shapes=[
            pltpu.VMEM((halves, z.RP, z.C, LANES), F32),
            pltpu.VMEM((z.ND, 3, z.HD, z.F), BF16),
            pltpu.VMEM((halves, z.VL * z.PR, LANES), F32),
            pltpu.VMEM((3, z.H, z.F), F32),
            dma((halves,)), dma((halves + 1,)),
        ],
        compiler_params=pltpu.CompilerParams(vmem_limit_bytes=40 * 1024 * 1024),
    )(state, grads.reshape(z.ND, 3, z.HD, z.F))
    return grad_state.reshape(final_cot.shape), grad_in, grad_out, grad_bias[0]


def solution(mesh):
    placed = (
        P(None, None, "lev", None, "band", None),
        P(None, "lev", None, "band", None),
        P(None, None, None, "band", "lev"),
        P(),
        P(),
        P("band", None, None),
        P(),
        P(),
        P(),
    )
    return jax.shard_map(
        shards,
        mesh=mesh,
        in_specs=placed,
        out_specs=(P(None, "lev", None, "band", None), P(), P(), P()),
        check_vma=False,
    )
```

```python
import functools

import jax
import jax.numpy as jnp
from jax import lax
from jax.experimental import pallas as pl
from jax.experimental.pallas import tpu as pltpu
from jax.sharding import PartitionSpec as P

dt_scale = 1.0
F32 = jnp.float32
BF16 = jnp.bfloat16
MESH = pl.DeviceIdType.MESH
LANES = 128


def dot(a, b):
    return jnp.dot(a, b, preferred_element_type=F32)


def dot_nt(a, b):
    return lax.dot_general(a, b, (((1,), (1,)), ((), ())), preferred_element_type=F32)


class Sizes:
    def __init__(self, bands, levs, steps, fields, levels, waves, wave_count, lat, lon, nobs, hidden):
        self.B, self.LV, self.S, self.NO = bands, levs, steps, nobs
        self.V, self.L, self.R, self.N = fields, levels, waves, wave_count
        self.J, self.O, self.H = lat, lon, hidden
        self.RP = waves // 2
        self.RT = self.RP * bands
        self.PR = 2 * waves + 8
        self.JJ = min(16, lat)
        self.Q = lat // self.JJ
        self.VL = fields * levels
        self.C = 4 * self.VL
        self.F = self.VL * levs
        self.ND = bands * levs
        self.HD = hidden // self.ND
        self.PITCH = self.JJ + 8
        self.OPITCH = self.F + 8
        self.ROWS = self.VL * 2 * waves
        self.G = min(8, self.JJ)
        self.HC = min(256, hidden)
        self.joint = lat % (8 * levs) == 0 and self.RP % 4 == 0
        if self.joint:
            self.JD, self.JQ, self.RG = lat // levs, 4, 4
            self.Q = self.JD // self.JQ


def kernel(
    z, ck, fc, obs, leg, obs_time, wave, w_in_raw, w_out_raw, bias_raw,
    out, gout,
    tab_t, tab_w, w_in_t, w_in, w_out, bias, orders, damp,
    tab, adj, tsend, trecv, fsend, frecv, bsend, brecv,
    lf_send, lf_recv, lt_send, lt_recv, lg_send, lg_recv,
    fs, fs2, cstage, ostage, obs_all, obs_s, acc_in, acc_out, acc_b,
    rs_send, rs_recv, ag_send, ag_recv,
    t_s, t_r, f_s, f_r, b_s, b_r, lf_s, lf_r, lt_s, lt_r, lg_s, lg_r, rs_s, rs_r, ag_s, ag_r,
    ck_sem, fc_sem, obs_sem, leg_sem, out_sem, g_sem,
):
    me_b = lax.axis_index("band")
    me_l = lax.axis_index("lev")
    me = me_b * z.LV + me_l

    def to_band(src, dst, ssem, rsem, b):
        return pltpu.make_async_remote_copy(
            src_ref=src, dst_ref=dst, send_sem=ssem, recv_sem=rsem,
            device_id=(b, me_l), device_id_type=MESH,
        )

    def to_lev(src, dst, ssem, rsem, v):
        return pltpu.make_async_remote_copy(
            src_ref=src, dst_ref=dst, send_sem=ssem, recv_sem=rsem,
            device_id=(me_b, v), device_id_type=MESH,
        )

    def others(count, own, body):
        def step(d, _):
            off = d + 1
            body(lax.rem(own + off, count))
            return 0

        lax.fori_loop(0, count - 1, step, 0)

    def band_send(send, recv, ssem, rsem, q):
        others(z.B, me_b, lambda b: to_band(
            send.at[b, q], recv.at[me_b, q], ssem.at[q, b], rsem.at[q, me_b], b).start())
        recv[me_b, q] = send[me_b, q]

    def band_wait_recv(send, recv, ssem, rsem, q):
        others(z.B, me_b, lambda b: to_band(
            send.at[b, q], recv.at[b, q], ssem.at[q, b], rsem.at[q, b], b).wait_recv())

    def band_wait_send(send, recv, ssem, rsem, q):
        others(z.B, me_b, lambda b: to_band(
            send.at[b, q], recv.at[b, q], ssem.at[q, b], rsem.at[q, b], b).wait_send())

    def feat_send(par, q):
        others(z.B, me_b, lambda b: to_band(
            fsend.at[b, q], frecv.at[par, me_b, q], f_s.at[q, b], f_r.at[par, q, me_b], b).start())
        frecv[par, me_b, q] = fsend[me_b, q]

    def feat_wait_recv(par, q):
        others(z.B, me_b, lambda b: to_band(
            fsend.at[b, q], frecv.at[par, b, q], f_s.at[q, b], f_r.at[par, q, b], b).wait_recv())

    def feat_wait_send():
        for q in range(z.Q):
            others(z.B, me_b, lambda b: to_band(
                fsend.at[b, q], frecv.at[0, b, q], f_s.at[q, b], f_r.at[0, q, b], b).wait_send())

    def lev_send(send, recv, ssem, rsem, q):
        others(z.LV, me_l, lambda v: to_lev(
            send.at[v, q], recv.at[me_l, q], ssem.at[q, v], rsem.at[q, me_l], v).start())
        recv[me_l, q] = send[me_l, q]

    def lev_wait_recv(send, recv, ssem, rsem, q):
        others(z.LV, me_l, lambda v: to_lev(
            send.at[v, q], recv.at[v, q], ssem.at[q, v], rsem.at[q, v], v).wait_recv())

    def lev_wait_send(send, recv, ssem, rsem, q):
        others(z.LV, me_l, lambda v: to_lev(
            send.at[v, q], recv.at[v, q], ssem.at[q, v], rsem.at[q, v], v).wait_send())

    def ck_copy(k, h):
        return pltpu.make_async_copy(
            ck.at[k, :, pl.ds(h * LANES, LANES)], cstage.at[h], ck_sem.at[h])

    def fc_copy(h):
        return pltpu.make_async_copy(
            fc.at[:, pl.ds(h * LANES, LANES)], ostage.at[h], fc_sem.at[h])

    halves = z.N // LANES
    bj = z.B * z.JJ
    if z.Q == 1:
        leg_copies = [pltpu.make_async_copy(leg, tab.at[:, 0], leg_sem.at[0])]
    else:
        leg_copies = [
            pltpu.make_async_copy(
                leg.at[:, pl.ds(b * z.J + q * z.JJ, z.JJ), :],
                tab.at[:, q, pl.ds(b * z.JJ, z.JJ), :],
                leg_sem.at[b * z.Q + q],
            )
            for b in range(z.B)
            for q in range(z.Q)
        ]
    obs_copy = pltpu.make_async_copy(obs, obs_all, obs_sem.at[0])
    for h in range(halves):
        ck_copy(z.S - 1, h).start()
    for c in leg_copies:
        c.start()
    for h in range(halves):
        fc_copy(h).start()
    obs_copy.start()

    half_c = 2 * z.VL
    degree = lax.broadcasted_iota(jnp.int32, (half_c, z.N), 1)

    def upper(rp, r2):
        return degree >= wave[me_b * z.R + 2 * rp + r2]

    def rows_of(stage, rp):
        parts = []
        for r2 in range(2):
            for p in range(2):
                start = p * z.R + 2 * rp + r2
                parts.append(jnp.concatenate(
                    [stage[h, pl.ds(start, z.VL, stride=2 * z.R), :] for h in range(halves)], axis=1))
        return jnp.concatenate(parts, axis=0)

    lane = lax.broadcasted_iota(jnp.int32, (z.Q * bj, z.C), 1)

    def legendre(s, rp, send):
        masked = jnp.concatenate(
            [jnp.where(upper(rp, r2), s[r2 * half_c:(r2 + 1) * half_c], 0.0) for r2 in range(2)],
            axis=0).astype(BF16)
        sums = [dot_nt(tab[2 * rp + r2].reshape(z.Q * bj, z.N), masked) for r2 in range(2)]
        sums = jnp.where(lane < half_c, sums[0], sums[1])
        for q in range(z.Q):
            for b in range(z.B):
                row = q * bj + b * z.JJ
                send[b, q, rp] = sums[row:row + z.JJ].astype(BF16)

    def features_legendre():
        def body(rp, _):
            legendre(rows_of(cstage, rp), rp, fsend)
            return 0

        lax.fori_loop(0, z.RP, body, 0, unroll=2)

    def tangent_legendre():
        def body(rp, _):
            damped = damp[...] * adj[rp]
            adj[rp] = damped
            legendre(dt_scale * damped, rp, tsend)
            return 0

        lax.fori_loop(0, z.RP, body, 0, unroll=2)

    def fourier(recv, q, table, scale, send):
        def convert(b, _):
            block = recv[b, q].astype(F32)
            for rp in range(z.RP):
                row = pl.multiple_of((b * z.RP + rp) * z.PITCH, 8)
                fs[pl.ds(row, z.JJ), :] = block[rp]
            return 0

        lax.fori_loop(0, z.B, convert, 0)

        def group(g, _):
            parts = []
            for i in range(z.G):
                at = fs[pl.ds(g * z.G + i, z.RT, stride=z.PITCH), :].T.astype(BF16)
                parts.append(jnp.concatenate(
                    [at[c * z.VL:(c + 1) * z.VL] for c in range(4)], axis=1))
            y = dot(jnp.concatenate(parts, axis=0), table[...])
            if scale is not None:
                y = y * scale
            y = y.astype(BF16)
            for v in range(z.LV):
                for i in range(z.G):
                    send[v, q, g * z.G + i] = y[i * z.VL:(i + 1) * z.VL, v * z.O:(v + 1) * z.O]
            return 0

        lax.fori_loop(0, z.JJ // z.G, group, 0)

    def adjoint_fourier(q):
        def group(g, _):
            x = jnp.concatenate([
                jnp.concatenate([lg_recv[v, q, g * z.G + i] for v in range(z.LV)], axis=1)
                for i in range(z.G)], axis=0)
            y = dot_nt(x, tab_w[...])
            for i in range(z.G):
                yi = y[i * z.VL:(i + 1) * z.VL]
                st = jnp.concatenate([yi[:, c * z.RT:(c + 1) * z.RT] for c in range(4)], axis=0)
                fs2[pl.ds(g * z.G + i, z.RT, stride=z.PITCH), :] = st.T
            return 0

        lax.fori_loop(0, z.JJ // z.G, group, 0)

        def convert(b, _):
            for rp in range(z.RP):
                row = pl.multiple_of((b * z.RP + rp) * z.PITCH, 8)
                bsend[b, q, rp] = fs2[pl.ds(row, z.JJ), :].astype(BF16)
            return 0

        lax.fori_loop(0, z.B, convert, 0)

    def adjoint_legendre(q):
        def body(rp, _):
            b_t = jnp.concatenate(
                [brecv[b, q, rp].astype(F32) for b in range(z.B)], axis=0).T.astype(BF16)
            for r2 in range(2):
                rows = slice(r2 * half_c, (r2 + 1) * half_c)
                grad = dot(b_t[rows], tab[2 * rp + r2, q])
                adj[rp, rows] = adj[rp, rows] + jnp.where(upper(rp, r2), grad, 0.0)
            return 0

        lax.fori_loop(0, z.RP, body, 0, unroll=2)

    def observations(k):
        weights = [jnp.where(obs_time[i] == k, 1.0, 0.0).astype(F32) for i in range(z.NO)]

        def body(f, _):
            v, rest = f // z.LV // z.L, lax.rem(f, z.LV * z.L)
            row = (rest // z.L) * z.VL + v * z.L + lax.rem(rest, z.L)
            total = weights[0] * obs_all[0, f]
            for i in range(1, z.NO):
                total = total + weights[i] * obs_all[i, f]
            obs_s[pl.ds(row, z.J, stride=z.OPITCH), :] = total
            return 0

        lax.fori_loop(0, z.F, body, 0, unroll=4)

    ng = min(4, z.JJ)

    def network(q):
        def group(g, _):
            def columns(ref):
                return jnp.concatenate([
                    jnp.concatenate([ref[v, q, g * ng + i] for v in range(z.LV)], axis=0)
                    for i in range(ng)], axis=1)

            x = columns(lf_recv)
            t = columns(lt_recv)
            grad = None
            for h in range(0, z.H, z.HC):
                rows = slice(h, h + z.HC)
                b = bias[rows]
                pre = dot(w_in_t[rows], x) + jnp.concatenate([b] * ng, axis=1)
                logistic = 0.5 * jnp.tanh(0.5 * pre) + 0.5
                hid = pre * logistic
                pg = dot(w_out[rows], t) * (logistic + hid * (1.0 - logistic))
                low = pg.astype(BF16)
                acc_out[rows] += dot_nt(hid.astype(BF16), t)
                acc_in[rows] += dot_nt(low, x)
                total = pg[:, :z.O]
                for i in range(1, ng):
                    total = total + pg[:, i * z.O:(i + 1) * z.O]
                acc_b[rows] += total
                part = dot(w_in[:, rows], low)
                grad = part if grad is None else grad + part
            for i in range(ng):
                j = q * z.JJ + g * ng + i
                row = pl.multiple_of(j * z.OPITCH, 8)
                col = grad[:, i * z.O:(i + 1) * z.O] + obs_s[pl.ds(row, z.F), :]
                col = col.astype(BF16)
                for v in range(z.LV):
                    lg_send[v, q, g * ng + i] = col[v * z.VL:(v + 1) * z.VL]
            return 0

        lax.fori_loop(0, z.JJ // ng, group, 0)

    def prepare():
        def wire(w):
            return jnp.concatenate([
                w[(v * z.LV + l) * z.L:(v * z.LV + l + 1) * z.L]
                for l in range(z.LV) for v in range(z.V)], axis=0)

        wi = wire(w_in_raw[...].astype(F32))
        w_in[...] = wi.astype(BF16)
        w_in_t[...] = wi.T.astype(BF16)
        w_out[...] = wire(w_out_raw[...].astype(F32).T).T.astype(BF16)
        bias[...] = jnp.broadcast_to(bias_raw[...], (z.O, z.H)).T

        def fill(i, _):
            for r2 in range(2):
                orders[pl.ds(r2 * z.RT + i, 1), :] = jnp.full((1, LANES), wave[2 * i + r2], jnp.int32)
            return 0

        lax.fori_loop(0, z.RT, fill, 0, unroll=4)
        lon = z.O * z.LV
        for r2 in range(2):
            order = orders[r2 * z.RT:(r2 + 1) * z.RT]
            weight = jnp.where(order == 0, 1.0, 2.0).astype(F32)
            for tile in range(lon // LANES):
                cols = slice(tile * LANES, (tile + 1) * LANES)
                longitude = lax.broadcasted_iota(jnp.int32, (z.RT, LANES), 1) + tile * LANES
                turn = (order * longitude).astype(F32)
                turn = turn - jnp.floor(turn * (1.0 / lon)) * lon
                angle = (2.0 * jnp.pi / lon) * turn
                for p, value in enumerate((jnp.cos(angle), -jnp.sin(angle))):
                    rows = slice((2 * r2 + p) * z.RT, (2 * r2 + p + 1) * z.RT)
                    value = value.astype(BF16)
                    tab_t[rows, cols] = value
                    tab_w[rows, cols] = (value.astype(F32) * weight).astype(BF16)

    def to_device(src, dst, ssem, rsem, d):
        return pltpu.make_async_remote_copy(
            src_ref=src, dst_ref=dst, send_sem=ssem, recv_sem=rsem,
            device_id=(d // z.LV, lax.rem(d, z.LV)), device_id_type=MESH,
        )

    def reduce_send():
        for i, acc in enumerate((acc_in, acc_out, acc_b)):
            for d in range(z.ND):
                rs_send[d, i] = acc[d * z.HD:(d + 1) * z.HD].astype(BF16)
        rs_recv[me] = rs_send[me]
        others(z.ND, me, lambda d: to_device(
            rs_send.at[d], rs_recv.at[me], rs_s.at[d], rs_r.at[me], d).start())

    def gather_send():
        others(z.ND, me, lambda d: to_device(
            rs_send.at[d], rs_recv.at[d], rs_s.at[d], rs_r.at[d], d).wait())
        total = rs_recv[0].astype(F32)
        for d in range(1, z.ND):
            total = total + rs_recv[d].astype(F32)
        total = total.astype(BF16)
        ag_send[...] = total
        ag_recv[me] = total
        others(z.ND, me, lambda d: to_device(
            ag_send, ag_recv.at[me], ag_s.at[d], ag_r.at[me], d).start())

    def gather_wait():
        others(z.ND, me, lambda d: to_device(
            ag_send, ag_recv.at[d], ag_s.at[d], ag_r.at[d], d).wait())

    for h in range(halves):
        ck_copy(z.S - 1, h).wait()
    for c in leg_copies:
        c.wait()
    features_legendre()
    feat_send((z.S - 1) % 2, 0)
    if z.S > 1:
        for h in range(halves):
            ck_copy(z.S - 2, h).start()
    degrees = lax.broadcasted_iota(jnp.int32, (1, z.N), 1).astype(F32)
    damp[...] = 1.0 / (1.0 + 2.0 * degrees * (degrees + 1.0) / (z.N * z.N))
    for h in range(halves):
        fc_copy(h).wait()

    def initial(rp, _):
        adj[rp] = rows_of(ostage, rp)
        return 0

    lax.fori_loop(0, z.RP, initial, 0)

    tang = (tsend, trecv, t_s, t_r)
    back = (bsend, brecv, b_s, b_r)
    lt = (lt_send, lt_recv, lt_s, lt_r)
    lf = (lf_send, lf_recv, lf_s, lf_r)
    lg = (lg_send, lg_recv, lg_s, lg_r)

    tangent_legendre()
    for q in range(z.Q):
        if q > 0:
            feat_send((z.S - 1) % 2, q)
        band_send(*tang, q)
    acc_in[...] = jnp.zeros_like(acc_in)
    acc_out[...] = jnp.zeros_like(acc_out)
    acc_b[...] = jnp.zeros_like(acc_b)
    prepare()
    obs_copy.wait()

    def step(i, _):
        k = z.S - 1 - i
        par = lax.rem(k, 2)

        def do_f(q):
            feat_wait_recv(par, q)
            fourier(frecv.at[par], q, tab_w, None, lf_send)
            lev_send(*lf, q)

        def do_t(q):
            band_wait_recv(*tang, q)
            fourier(trecv, q, tab_t, 1.0 / (z.O * z.LV), lt_send)
            lev_send(*lt, q)

        def do_n(q):
            lev_wait_recv(*lf, q)
            lev_wait_recv(*lt, q)
            network(q)
            lev_send(*lg, q)

        def do_b(q):
            lev_wait_recv(*lg, q)

            @pl.when(i > 0)
            def _():
                band_wait_send(*back, q)

            adjoint_fourier(q)
            band_send(*back, q)

        do_f(0)

        @pl.when(k > 0)
        def _():
            for h in range(halves):
                ck_copy(k - 1, h).wait()
            feat_wait_send()
            features_legendre()
            feat_send(1 - par, 0)

        @pl.when(k > 1)
        def _():
            for h in range(halves):
                ck_copy(k - 2, h).start()

        observations(k)
        do_t(0)
        for q in range(1, z.Q):
            do_f(q)
        do_n(0)
        for q in range(1, z.Q):
            do_t(q)
            do_b(q - 1)
            do_n(q)

        @pl.when(k == 0)
        def _():
            reduce_send()

        do_b(z.Q - 1)

        @pl.when(k > 0)
        def _():
            for q in range(1, z.Q):
                feat_send(1 - par, q)

        @pl.when(k == 0)
        def _():
            gather_send()

        for q in range(z.Q):
            band_wait_recv(*back, q)
            adjoint_legendre(q)
        for q in range(z.Q):
            band_wait_send(*tang, q)

        @pl.when(k > 0)
        def _():
            tangent_legendre()
            for q in range(z.Q):
                band_send(*tang, q)

        for q in range(z.Q):
            lev_wait_send(*lf, q)
            lev_wait_send(*lt, q)
            lev_wait_send(*lg, q)
        return 0

    lax.fori_loop(0, z.S, step, 0)
    adj_copy = pltpu.make_async_copy(adj, out, out_sem.at[0])
    adj_copy.start()
    gather_wait()
    gather_copy = pltpu.make_async_copy(ag_recv, gout, g_sem.at[0])
    gather_copy.start()
    feat_wait_send()
    for q in range(z.Q):
        band_wait_send(*back, q)
    adj_copy.wait()
    gather_copy.wait()


def joint_kernel(
    z, ck, fc, obs, leg, obs_time, wave, w_in_raw, w_out_raw, bias_raw,
    out, gout,
    tab_t, tab_w, w_in_t, w_in, w_out, bias, orders, damp,
    tab, adj, tsend, trecv, fsend, frecv, bsend, brecv, osend, orecv,
    feats, tangs, fs, fs2, cstage, ostage, obs_all, obs_s, acc_in, acc_out, acc_b,
    rs_send, rs_recv, rb_send, rb_recv, ag_send, gb_recv, ag_recv,
    t_s, t_r, f_s, f_r, b_s, b_r, o_s, o_r, rl_s, rl_r, rb_s, rb_r,
    ck_sem, fc_sem, obs_sem, leg_sem, out_sem, g_sem,
):
    me_b = lax.axis_index("band")
    me_l = lax.axis_index("lev")
    me = me_b * z.LV + me_l
    halves = z.N // LANES
    lon = z.O * z.LV
    half_c = 2 * z.VL

    def others(count, own, body):
        def step(d, _):
            body(lax.rem(own + d, count))
            return 0

        lax.fori_loop(1, count, step, 0, unroll=min(4, count - 1))

    def remote(src, dst, ssem, rsem, d):
        return pltpu.make_async_remote_copy(
            src_ref=src, dst_ref=dst, send_sem=ssem, recv_sem=rsem,
            device_id=(d // z.LV, lax.rem(d, z.LV)), device_id_type=MESH,
        )

    def send_all(send, recv, ssem, rsem, q):
        others(z.ND, me, lambda d: remote(
            send.at[d, q], recv.at[me, q], ssem.at[q, d], rsem.at[q, me], d).start())
        recv[me, q] = send[me, q]

    def wait_recv(send, recv, ssem, rsem, q):
        others(z.ND, me, lambda d: remote(
            send.at[d, q], recv.at[d, q], ssem.at[q, d], rsem.at[q, d], d).wait_recv())

    def wait_send(send, recv, ssem, rsem, q):
        others(z.ND, me, lambda d: remote(
            send.at[d, q], recv.at[d, q], ssem.at[q, d], rsem.at[q, d], d).wait_send())

    def obs_send(par):
        others(z.LV, me_l, lambda v: remote(
            osend.at[v], orecv.at[par, me_l], o_s.at[v], o_r.at[par, me_l],
            me_b * z.LV + v).start())
        orecv[par, me_l] = osend[me_l]

    def obs_wait_recv(par):
        others(z.LV, me_l, lambda v: remote(
            osend.at[v], orecv.at[par, v], o_s.at[v], o_r.at[par, v],
            me_b * z.LV + v).wait_recv())

    def obs_wait_send():
        others(z.LV, me_l, lambda v: remote(
            osend.at[v], orecv.at[0, v], o_s.at[v], o_r.at[0, v],
            me_b * z.LV + v).wait_send())

    def stage_copies(src, stage, sem, h):
        def copy(v, _):
            pltpu.make_async_copy(
                src.at[pl.ds(v * 2 * z.R, 2 * z.R), pl.ds(h * LANES, LANES)],
                stage.at[h, pl.ds(v * z.PR, 2 * z.R)], sem.at[h]).start()
            return 0

        lax.fori_loop(0, z.VL, copy, 0)

    def stage_wait(src, stage, sem, h):
        pltpu.make_async_copy(
            src.at[:, pl.ds(h * LANES, LANES)], stage.at[h, pl.ds(0, z.ROWS)], sem.at[h]).wait()

    leg_copy = pltpu.make_async_copy(leg, tab, leg_sem.at[0])
    obs_copy = pltpu.make_async_copy(obs, obs_all, obs_sem.at[0])
    for h in range(halves):
        stage_copies(ck.at[z.S - 1], cstage, ck_sem, h)
    leg_copy.start()
    for h in range(halves):
        stage_copies(fc, ostage, fc_sem, h)
    obs_copy.start()

    degree = lax.broadcasted_iota(jnp.int32, (half_c, z.N), 1)

    def upper(rp, r2):
        return degree >= wave[me_b * z.R + 2 * rp + r2]

    def rows_of(stage, rp):
        parts = []
        for r2 in range(2):
            for p in range(2):
                start = p * z.R + 2 * rp + r2
                parts.append(jnp.concatenate(
                    [stage[h, pl.ds(start, z.VL, stride=z.PR), :] for h in range(halves)], axis=1))
        return jnp.concatenate(parts, axis=0)

    lat = z.ND * z.JD
    lane = lax.broadcasted_iota(jnp.int32, (lat, z.C), 1)

    def legendre(s, rp):
        masked = jnp.concatenate(
            [jnp.where(upper(rp, r2), s[r2 * half_c:(r2 + 1) * half_c], 0.0) for r2 in range(2)],
            axis=0).astype(BF16)
        sums = [dot_nt(tab[2 * rp + r2], masked) for r2 in range(2)]
        return jnp.where(lane < half_c, sums[0], sums[1]).reshape(z.ND, z.JD, z.C)

    def legendre_groups(spectral, send):
        def body(g, _):
            sums = [legendre(spectral(g * z.RG + i), g * z.RG + i) for i in range(z.RG)]
            row = pl.multiple_of(g * z.RG * z.JQ, z.RG * z.JQ)
            for q in range(z.Q):
                block = jnp.concatenate(
                    [s[:, q * z.JQ:(q + 1) * z.JQ] for s in sums], axis=1)
                send[:, q, pl.ds(row, z.RG * z.JQ), :] = block.astype(BF16)
            return 0

        lax.fori_loop(0, z.RP // z.RG, body, 0)

    def features_legendre():
        legendre_groups(lambda rp: rows_of(cstage, rp), fsend)

    def tangent_legendre():
        def damped(rp):
            value = damp[...] * adj[rp]
            adj[rp] = value
            return dt_scale * value

        legendre_groups(damped, tsend)

    block = z.RP * z.JQ

    def fourier(recv, q, table, scale, dst):
        def convert(b, _):
            for v in range(z.LV):
                row = pl.multiple_of((v * z.B + b) * block, block)
                fs[pl.ds(row, block), :] = recv[b * z.LV + v, q].astype(F32)
            return 0

        lax.fori_loop(0, z.B, convert, 0, unroll=2)
        parts = []
        for i in range(z.JQ):
            for v in range(z.LV):
                at = fs[pl.ds(v * z.B * block + i, z.RT, stride=z.JQ), :].T.astype(BF16)
                parts.append(jnp.concatenate(
                    [at[c * z.VL:(c + 1) * z.VL] for c in range(4)], axis=1))
        y = dot(jnp.concatenate(parts, axis=0), table[...])
        if scale is not None:
            y = y * scale
        y = y.astype(BF16)
        for i in range(z.JQ):
            dst[q * z.JQ + i] = y[i * z.F:(i + 1) * z.F]

    def network(q, par):
        def column(i, _):
            j = q * z.JQ + i
            x = feats[j]
            t = tangs[j]
            grad = None
            for h in range(0, z.H, z.HC):
                rows = slice(h, h + z.HC)
                pre = dot(w_in_t[rows], x) + jnp.concatenate([bias[rows]] * z.LV, axis=1)
                logistic = 0.5 * jnp.tanh(0.5 * pre) + 0.5
                hid = pre * logistic
                pg = dot(w_out[rows], t) * (logistic + hid * (1.0 - logistic))
                low = pg.astype(BF16)
                acc_out[rows] += dot_nt(hid.astype(BF16), t)
                acc_in[rows] += dot_nt(low, x)
                total = pg[:, :z.O]
                for v in range(1, z.LV):
                    total = total + pg[:, v * z.O:(v + 1) * z.O]
                acc_b[rows] += total
                part = dot(w_in[:, rows], low)
                grad = part if grad is None else grad + part
            grad = grad + jnp.concatenate(
                [orecv[par, v, j].astype(F32) for v in range(z.LV)], axis=1)
            y = dot_nt(grad.astype(BF16), tab_w[...])
            for v in range(z.LV):
                yv = y[v * z.VL:(v + 1) * z.VL]
                st = jnp.concatenate([yv[:, c * z.RT:(c + 1) * z.RT] for c in range(4)], axis=0)
                fs2[pl.ds(v * z.B * block + i, z.RT, stride=z.JQ), :] = st.T
            return 0

        lax.fori_loop(0, z.JQ, column, 0)

        def convert(b, _):
            for v in range(z.LV):
                row = pl.multiple_of((v * z.B + b) * block, block)
                bsend[b * z.LV + v, q] = fs2[pl.ds(row, block), :].astype(BF16)
            return 0

        lax.fori_loop(0, z.B, convert, 0, unroll=2)

    def adjoint_legendre():
        def body(g, _):
            row = pl.multiple_of(g * z.RG * z.JQ, z.RG * z.JQ)
            chunks = [brecv[:, q, pl.ds(row, z.RG * z.JQ), :].astype(F32) for q in range(z.Q)]
            for i in range(z.RG):
                rp = g * z.RG + i
                b_t = jnp.concatenate(
                    [c[:, i * z.JQ:(i + 1) * z.JQ] for c in chunks],
                    axis=1).reshape(lat, z.C).T.astype(BF16)
                for r2 in range(2):
                    rows = slice(r2 * half_c, (r2 + 1) * half_c)
                    grad = dot(b_t[rows], tab[2 * rp + r2])
                    adj[rp, rows] = adj[rp, rows] + jnp.where(upper(rp, r2), grad, 0.0)
            return 0

        lax.fori_loop(0, z.RP // z.RG, body, 0)

    def observations(k):
        weights = [jnp.where(obs_time[i] == k, 1.0, 0.0).astype(F32) for i in range(z.NO)]

        def body(f, _):
            v, rest = f // z.LV // z.L, lax.rem(f, z.LV * z.L)
            row = (rest // z.L) * z.VL + v * z.L + lax.rem(rest, z.L)
            total = weights[0] * obs_all[0, f]
            for i in range(1, z.NO):
                total = total + weights[i] * obs_all[i, f]
            obs_s[pl.ds(row, z.J, stride=z.OPITCH), :] = total
            return 0

        lax.fori_loop(0, z.F, body, 0, unroll=4)

        def pack(v, _):
            for j in range(z.JD):
                row = pl.multiple_of((v * z.JD + j) * z.OPITCH, 8)
                osend[v, j] = obs_s[pl.ds(row, z.F), :].astype(BF16)
            return 0

        lax.fori_loop(0, z.LV, pack, 0)

    def prepare():
        def wire(w):
            return jnp.concatenate([
                w[(v * z.LV + l) * z.L:(v * z.LV + l + 1) * z.L]
                for l in range(z.LV) for v in range(z.V)], axis=0)

        wi = wire(w_in_raw[...].astype(F32))
        w_in[...] = wi.astype(BF16)
        w_in_t[...] = wi.T.astype(BF16)
        w_out[...] = wire(w_out_raw[...].astype(F32).T).T.astype(BF16)
        bias[...] = jnp.broadcast_to(bias_raw[...], (z.O, z.H)).T

        def fill(i, _):
            for r2 in range(2):
                orders[pl.ds(r2 * z.RT + i, 1), :] = jnp.full((1, LANES), wave[2 * i + r2], jnp.int32)
            return 0

        lax.fori_loop(0, z.RT, fill, 0, unroll=4)
        for r2 in range(2):
            order = orders[r2 * z.RT:(r2 + 1) * z.RT]
            weight = jnp.where(order == 0, 1.0, 2.0).astype(F32)
            for tile in range(lon // LANES):
                cols = slice(tile * LANES, (tile + 1) * LANES)
                longitude = lax.broadcasted_iota(jnp.int32, (z.RT, LANES), 1) + tile * LANES
                turn = (order * longitude).astype(F32)
                turn = turn - jnp.floor(turn * (1.0 / lon)) * lon
                angle = (2.0 * jnp.pi / lon) * turn
                for p, value in enumerate((jnp.cos(angle), -jnp.sin(angle))):
                    rows = slice((2 * r2 + p) * z.RT, (2 * r2 + p + 1) * z.RT)
                    value = value.astype(BF16)
                    tab_t[rows, cols] = value
                    tab_w[rows, cols] = (value.astype(F32) * weight).astype(BF16)

    def lev_copy(src, dst, stage, mine, v):
        return remote(src, dst, rl_s.at[stage, v], rl_r.at[stage, mine], me_b * z.LV + v)

    def band_copy(src, dst, stage, mine, b):
        return remote(src, dst, rb_s.at[stage, b], rb_r.at[stage, mine], b * z.LV + me_l)

    def reduce_lev():
        for i, acc in enumerate((acc_in, acc_out, acc_b)):
            for v in range(z.LV):
                for b in range(z.B):
                    row = (v * z.B + b) * z.HD
                    rs_send[v, b, i] = acc[row:row + z.HD].astype(BF16)
        rs_recv[me_l] = rs_send[me_l]
        others(z.LV, me_l, lambda v: lev_copy(
            rs_send.at[v], rs_recv.at[me_l], 0, me_l, v).start())

    def reduce_band():
        others(z.LV, me_l, lambda v: lev_copy(
            rs_send.at[v], rs_recv.at[v], 0, v, v).wait())

        def add(b, _):
            total = rs_recv[0, b].astype(F32)
            for v in range(1, z.LV):
                total = total + rs_recv[v, b].astype(F32)
            rb_send[b] = total.astype(BF16)
            return 0

        lax.fori_loop(0, z.B, add, 0)
        rb_recv[me_b] = rb_send[me_b]
        others(z.B, me_b, lambda b: band_copy(
            rb_send.at[b], rb_recv.at[me_b], 0, me_b, b).start())

    def gather_band():
        others(z.B, me_b, lambda b: band_copy(
            rb_send.at[b], rb_recv.at[b], 0, b, b).wait())
        total = rb_recv[0].astype(F32)
        for b in range(1, z.B):
            total = total + rb_recv[b].astype(F32)
        total = total.astype(BF16)
        ag_send[...] = total
        gb_recv[me_b] = total
        others(z.B, me_b, lambda b: band_copy(
            ag_send, gb_recv.at[me_b], 1, me_b, b).start())

    def gather_lev():
        others(z.B, me_b, lambda b: band_copy(
            ag_send, gb_recv.at[b], 1, b, b).wait())
        ag_recv[me_l] = gb_recv[...]
        others(z.LV, me_l, lambda v: lev_copy(
            gb_recv, ag_recv.at[me_l], 1, me_l, v).start())

    def gather_wait():
        others(z.LV, me_l, lambda v: lev_copy(
            gb_recv, ag_recv.at[v], 1, v, v).wait())

    for h in range(halves):
        stage_wait(ck.at[z.S - 1], cstage, ck_sem, h)
    leg_copy.wait()
    tang = (tsend, trecv, t_s, t_r)
    back = (bsend, brecv, b_s, b_r)

    def feat(par):
        return (fsend, frecv.at[par], f_s, f_r.at[par])

    features_legendre()
    first = (z.S - 1) % 2
    send_all(*feat(first), 0)
    if z.S > 1:
        for h in range(halves):
            stage_copies(ck.at[z.S - 2], cstage, ck_sem, h)
    degrees = lax.broadcasted_iota(jnp.int32, (1, z.N), 1).astype(F32)
    damp[...] = 1.0 / (1.0 + 2.0 * degrees * (degrees + 1.0) / (z.N * z.N))
    for h in range(halves):
        stage_wait(fc, ostage, fc_sem, h)

    def initial(rp, _):
        adj[rp] = rows_of(ostage, rp)
        return 0

    lax.fori_loop(0, z.RP, initial, 0)
    tangent_legendre()
    for q in range(z.Q):
        if q > 0:
            send_all(*feat(first), q)
        send_all(*tang, q)
    obs_copy.wait()
    observations(z.S - 1)
    obs_send(first)
    acc_in[...] = jnp.zeros_like(acc_in)
    acc_out[...] = jnp.zeros_like(acc_out)
    acc_b[...] = jnp.zeros_like(acc_b)
    prepare()

    def step(i, _):
        k = z.S - 1 - i
        par = lax.rem(k, 2)

        def do_f(q):
            wait_recv(*feat(par), q)
            fourier(frecv.at[par], q, tab_w, None, feats)

        def do_n(q):
            wait_recv(*tang, q)
            fourier(trecv, q, tab_t, 1.0 / lon, tangs)
            if q == 0:
                obs_wait_recv(par)

            @pl.when(i > 0)
            def _():
                wait_send(*back, q)

            network(q, par)
            if q == z.Q - 1:
                @pl.when(k == 0)
                def _():
                    reduce_lev()

            send_all(*back, q)

        do_f(0)

        @pl.when(k > 0)
        def _():
            for h in range(halves):
                stage_wait(ck.at[k - 1], cstage, ck_sem, h)
            for q in range(z.Q):
                wait_send(*feat(0), q)
            features_legendre()
            send_all(*feat(1 - par), 0)

        @pl.when(k > 1)
        def _():
            for h in range(halves):
                stage_copies(ck.at[k - 2], cstage, ck_sem, h)

        do_n(0)

        @pl.when(k > 0)
        def _():
            obs_wait_send()
            observations(k - 1)
            obs_send(1 - par)

        for q in range(1, z.Q):
            do_f(q)
            do_n(q)

        @pl.when(k > 0)
        def _():
            for q in range(1, z.Q):
                send_all(*feat(1 - par), q)

        @pl.when(k == 0)
        def _():
            reduce_band()

        for q in range(z.Q):
            wait_recv(*back, q)

        @pl.when(k == 0)
        def _():
            gather_band()

        adjoint_legendre()
        for q in range(z.Q):
            wait_send(*tang, q)

        @pl.when(k > 0)
        def _():
            tangent_legendre()
            for q in range(z.Q):
                send_all(*tang, q)

        return 0

    lax.fori_loop(0, z.S, step, 0)
    adj_copy = pltpu.make_async_copy(adj, out, out_sem.at[0])
    adj_copy.start()
    gather_lev()
    gather_wait()
    gather_copy = pltpu.make_async_copy(ag_recv, gout, g_sem.at[0])
    gather_copy.start()
    obs_wait_send()
    for q in range(z.Q):
        wait_send(*feat(0), q)
        wait_send(*back, q)
    adj_copy.wait()
    gather_copy.wait()


def finish(z, adj_hbm, grads_hbm, out, grad_in, grad_out, grad_bias, adj, grads, stage, flat, sem, in_sem):
    half_c = 2 * z.VL
    halves = z.N // LANES
    grads_copy = pltpu.make_async_copy(grads_hbm, grads, in_sem.at[halves])
    adj_copies = [
        pltpu.make_async_copy(adj_hbm.at[:, :, pl.ds(h * LANES, LANES)], adj.at[h], in_sem.at[h])
        for h in range(halves)
    ]
    for copy in adj_copies:
        copy.start()
    grads_copy.start()
    for h in range(halves):
        adj_copies[h].wait()

        def body(rp, _):
            for r2 in range(2):
                for p in range(2):
                    start = p * z.R + 2 * rp + r2
                    c = r2 * half_c + p * z.VL
                    stage[h, pl.ds(start, z.VL, stride=z.PR), :] = adj[h, rp, c:c + z.VL]
            return 0

        lax.fori_loop(0, z.RP, body, 0, unroll=2)

        def store(v, _):
            pltpu.make_async_copy(
                stage.at[h, pl.ds(v * z.PR, 2 * z.R)],
                out.at[pl.ds(v * 2 * z.R, 2 * z.R), pl.ds(h * LANES, LANES)], sem.at[h]).start()
            return 0

        lax.fori_loop(0, z.VL, store, 0)

    grads_copy.wait()
    for d in range(z.ND):
        for i in range(3):
            flat[i, d * z.HD:(d + 1) * z.HD] = grads[d, i].astype(F32)

    def from_wire(w):
        return jnp.concatenate([
            w[(l * z.V + v) * z.L:(l * z.V + v + 1) * z.L]
            for v in range(z.V) for l in range(z.LV)], axis=0)

    grad_in[...] = from_wire(flat[0].T)
    grad_out[...] = from_wire(flat[1].T).T
    grad_bias[...] = jnp.sum(flat[2].T, axis=0, keepdims=True)
    for h in range(halves):
        pltpu.make_async_copy(
            stage.at[h, pl.ds(0, z.ROWS)], out.at[:, pl.ds(h * LANES, LANES)], sem.at[h]).wait()


def shards(checkpoints, final_cot, obs_cot, obs_time, wave_order, legendre, w_in, w_out, bias):
    local_waves, lat_count, wave_count = legendre.shape
    fields, levels = final_cot.shape[:2]
    z = Sizes(
        lax.axis_size("band"), lax.axis_size("lev"), checkpoints.shape[0], fields, levels,
        local_waves, wave_count, obs_cot.shape[3], obs_cot.shape[4], obs_cot.shape[0],
        w_in.shape[1])
    any_space = pl.BlockSpec(memory_space=pl.ANY)
    smem = pl.BlockSpec(memory_space=pltpu.SMEM)
    vmem = pl.BlockSpec(memory_space=pltpu.VMEM)
    dma = pltpu.SemaphoreType.DMA
    halves = z.N // LANES
    reduce_buf = pltpu.VMEM((z.ND, 3, z.HD, z.F), BF16)
    lon = z.O * z.LV
    weights = [
        pltpu.VMEM((4 * z.RT, lon), BF16), pltpu.VMEM((4 * z.RT, lon), BF16),
        pltpu.VMEM((z.H, z.F), BF16), pltpu.VMEM((z.F, z.H), BF16), pltpu.VMEM((z.H, z.F), BF16),
        pltpu.VMEM((z.H, z.O), F32), pltpu.VMEM((2 * z.RT, LANES), jnp.int32), pltpu.VMEM((1, z.N), F32),
    ]
    stage_rows = z.VL * z.PR if z.joint else z.ROWS
    stages = [
        pltpu.VMEM((halves, stage_rows, LANES), F32),
        pltpu.VMEM((halves, stage_rows, LANES), F32),
        pltpu.VMEM((z.NO, z.F, z.J, z.O), F32),
        pltpu.VMEM((z.J * z.OPITCH, z.O), F32),
        pltpu.VMEM((z.H, z.F), F32), pltpu.VMEM((z.H, z.F), F32), pltpu.VMEM((z.H, z.O), F32),
    ]
    part = pltpu.VMEM((3, z.HD, z.F), BF16)
    grads_shape = (z.ND, 3, z.HD, z.F)
    if z.joint:
        body = joint_kernel
        grads_shape = (z.LV, z.B, 3, z.HD, z.F)
        reduce_buf = pltpu.VMEM(grads_shape, BF16)
        band_part = pltpu.VMEM(grads_shape[1:], BF16)
        block = (z.ND, z.Q, z.RP * z.JQ, z.C)
        buf = pltpu.VMEM(block, BF16)
        obs_buf = (z.LV, z.JD, z.F, z.O)
        flat = pltpu.VMEM((z.ND * z.RP * z.JQ, z.C), F32)
        columns = pltpu.VMEM((z.JD, z.F, lon), BF16)
        pair = dma((z.Q, z.ND))
        scratch = weights + [
            pltpu.VMEM((z.R, z.ND * z.JD, z.N), BF16),
            pltpu.VMEM((z.RP, z.C, z.N), F32),
            buf, buf, buf, pltpu.VMEM((2,) + block, BF16), buf, buf,
            pltpu.VMEM(obs_buf, BF16), pltpu.VMEM((2,) + obs_buf, BF16),
            columns, columns, flat, flat,
        ] + stages + [
            reduce_buf, reduce_buf, band_part, band_part, part, band_part, reduce_buf,
            pair, pair, pair, dma((2, z.Q, z.ND)), pair, pair,
            dma((z.LV,)), dma((2, z.LV)),
            dma((2, z.LV)), dma((2, z.LV)), dma((2, z.B)), dma((2, z.B)),
            dma((halves,)), dma((halves,)), dma((1,)), dma((1,)), dma((1,)), dma((1,)),
        ]
    else:
        body = kernel
        band_buf = pltpu.VMEM((z.B, z.Q, z.RP, z.JJ, z.C), BF16)
        lev_buf = pltpu.VMEM((z.LV, z.Q, z.JJ, z.VL, z.O), BF16)
        flat = pltpu.VMEM((z.RT * z.PITCH, z.C), F32)
        scratch = weights + [
            pltpu.VMEM((z.R, z.Q, z.B * z.JJ, z.N), BF16),
            pltpu.VMEM((z.RP, z.C, z.N), F32),
            band_buf, band_buf, band_buf,
            pltpu.VMEM((2, z.B, z.Q, z.RP, z.JJ, z.C), BF16),
            band_buf, band_buf,
            lev_buf, lev_buf, lev_buf, lev_buf, lev_buf, lev_buf,
            flat, flat,
        ] + stages + [
            reduce_buf, reduce_buf, part, reduce_buf,
            dma((z.Q, z.B)), dma((z.Q, z.B)), dma((z.Q, z.B)), dma((2, z.Q, z.B)),
            dma((z.Q, z.B)), dma((z.Q, z.B)),
            dma((z.Q, z.LV)), dma((z.Q, z.LV)), dma((z.Q, z.LV)), dma((z.Q, z.LV)),
            dma((z.Q, z.LV)), dma((z.Q, z.LV)),
            dma((z.ND,)), dma((z.ND,)), dma((z.ND,)), dma((z.ND,)),
            dma((halves,)), dma((halves,)), dma((1,)), dma((z.B * z.Q,)), dma((1,)), dma((1,)),
        ]
    state, grads = pl.pallas_call(
        functools.partial(body, z),
        out_shape=[
            jax.ShapeDtypeStruct((z.RP, z.C, z.N), F32),
            jax.ShapeDtypeStruct(grads_shape, BF16),
        ],
        in_specs=[any_space] * 4 + [smem] * 2 + [vmem] * 3,
        out_specs=[any_space, any_space],
        scratch_shapes=scratch,
        compiler_params=pltpu.CompilerParams(
            has_side_effects=True, vmem_limit_bytes=60 * 1024 * 1024),
    )(
        checkpoints.reshape(z.S, z.ROWS, z.N),
        final_cot.reshape(z.ROWS, z.N),
        obs_cot.reshape(z.NO, z.F, z.J, z.O),
        legendre,
        obs_time, wave_order, w_in, w_out, bias[None],
    )
    grad_state, grad_in, grad_out, grad_bias = pl.pallas_call(
        functools.partial(finish, z),
        out_shape=[
            jax.ShapeDtypeStruct((z.ROWS, z.N), F32),
            jax.ShapeDtypeStruct((z.F, z.H), F32),
            jax.ShapeDtypeStruct((z.H, z.F), F32),
            jax.ShapeDtypeStruct((1, z.H), F32),
        ],
        in_specs=[any_space, any_space],
        out_specs=[any_space, vmem, vmem, vmem],
        scratch_shapes=[
            pltpu.VMEM((halves, z.RP, z.C, LANES), F32),
            pltpu.VMEM((z.ND, 3, z.HD, z.F), BF16),
            pltpu.VMEM((halves, z.VL * z.PR, LANES), F32),
            pltpu.VMEM((3, z.H, z.F), F32),
            dma((halves,)), dma((halves + 1,)),
        ],
        compiler_params=pltpu.CompilerParams(vmem_limit_bytes=40 * 1024 * 1024),
    )(state, grads.reshape(z.ND, 3, z.HD, z.F))
    return grad_state.reshape(final_cot.shape), grad_in, grad_out, grad_bias[0]


def solution(mesh):
    placed = (
        P(None, None, "lev", None, "band", None),
        P(None, "lev", None, "band", None),
        P(None, None, None, "band", "lev"),
        P(),
        P(),
        P("band", None, None),
        P(),
        P(),
        P(),
    )
    return jax.shard_map(
        shards,
        mesh=mesh,
        in_specs=placed,
        out_specs=(P(None, "lev", None, "band", None), P(), P(), P()),
        check_vma=False,
    )
```
